256 devices in a mesh: dp: 16 (over x, y), mp: 16 (over z, core).
Axes of the slice: x: 4, y: 4, z: 8, core: 2. Of those that a mesh axis runs over, the one named last changes fastest.
Arguments:
- query_grads: bfloat16 [16, 1, 3584, 4096], P('dp', None, None, 'mp'), may hold values from -102 to 102
- merge_grads: bfloat16 [16, 1, 4096, 3584], P('dp', None, 'mp'), may hold values from -102 to 102
- query_accum: float32 [1, 3584, 4096], P(None, 'dp', 'mp'), may hold values from -406 to 406
- merge_accum: float32 [1, 4096, 3584], P(None, 'mp', 'dp'), may hold values from -406 to 406
- query_master: float32 [1, 3584, 4096], P(None, 'dp', 'mp'), may hold values from -0.75 to 0.75
- merge_master: float32 [1, 4096, 3584], P(None, 'mp', 'dp'), may hold values from -0.75 to 0.75
- query_moment: float32 [1, 3584, 4096], P(None, 'dp', 'mp'), may hold values from -6 to 6
- merge_moment: float32 [1, 4096, 3584], P(None, 'mp', 'dp'), may hold values from -6 to 6
- query_second: float32 [1, 3584, 4096], P(None, 'dp', 'mp'), may hold values from 0.3 to 3
- merge_second: float32 [1, 4096, 3584], P(None, 'mp', 'dp'), may hold values from 0.3 to 3
Outputs:
- query_weight: bfloat16 [1, 3584, 4096], P(None, None, 'mp')
- merge_weight: bfloat16 [1, 4096, 3584], P(None, 'mp')
- query_shard: float32 [1, 3584, 4096], P(None, 'dp', 'mp')
- merge_shard: float32 [1, 4096, 3584], P(None, 'mp', 'dp')
- query_first: float32 [1, 3584, 4096], P(None, 'dp', 'mp')
- merge_first: float32 [1, 4096, 3584], P(None, 'mp', 'dp')
- query_variance: float32 [1, 3584, 4096], P(None, 'dp', 'mp')
- merge_variance: float32 [1, 4096, 3584], P(None, 'mp', 'dp')
The draws below stay inside these ranges and needn't reach their ends.
All inputs are finite; a program needn't handle non-finite values.
Results may differ from the reference program's by a relative error of at most 0.0015.
Values may be sent and summed in bfloat16 or wider, within the bound.
A program may use at most 64 MiB of HBM per device.

```python
import math
import jax
import jax.numpy as jnp
from jax import lax

D = 3584
HEADS = 16
HEAD_DIM = 256
LAYERS = 1
STEP = 10
QW = 4096
ENTRIES = 29360128
N_DP = 16


def scaled_field(key, tag, noise_tag, shape, base):
    rows = shape[-2]
    cols = shape[-1]
    scale_key = jax.random.fold_in(key, tag)
    row_rise = 1.0 + 0.75 * jnp.arange(rows, dtype=jnp.float32)[:, None] / rows
    col_rise = 1.0 + 0.75 * jnp.arange(cols, dtype=jnp.float32)[None, :] / cols
    row_shape = tuple(shape[:-1]) + (1,)
    col_shape = tuple(shape[:-2]) + (1, cols)
    row_scale = jnp.exp(jax.random.uniform(jax.random.fold_in(scale_key, 1), row_shape, jnp.float32) * math.log(10.0)) * row_rise
    col_scale = jnp.exp(jax.random.uniform(jax.random.fold_in(scale_key, 2), col_shape, jnp.float32) * math.log(10.0)) * col_rise
    noise_key = jax.random.fold_in(key, noise_tag)
    value = jax.random.truncated_normal(noise_key, -4.0, 4.0, shape, jnp.float32)
    return base * value * row_scale * col_scale


def draw_query_grads(key, part):
    return scaled_field(key, 1, 5, (N_DP, LAYERS, D, HEADS * HEAD_DIM), 0.05).astype(jnp.bfloat16)


def draw_merge_grads(key, part):
    return scaled_field(key, 2, 6, (N_DP, LAYERS, HEADS * HEAD_DIM, D), 0.05).astype(jnp.bfloat16)


def draw_query_accum(key, part):
    return scaled_field(key, 3, 7, (LAYERS, D, HEADS * HEAD_DIM), 0.2)


def draw_merge_accum(key, part):
    return scaled_field(key, 4, 8, (LAYERS, HEADS * HEAD_DIM, D), 0.2)


def block_scale(key, extent, split, smallest, largest):
    level, own = 1.0, jax.random.fold_in(key, 6)
    for position, parts in split:
        draws = jnp.exp(jax.random.uniform(jax.random.fold_in(own, position), (parts,), jnp.float32, smallest / len(split), largest / len(split)))
        level = level * jnp.repeat(draws, extent[position] // parts).reshape([-1 if axis == position else 1 for axis in range(len(extent))])
    return level


def bell_draw(rng, shape, scale, most, pieces=(), kind=jnp.bfloat16):
    drawn = jax.random.normal(rng, shape, jnp.float32) * scale
    if len(pieces) > 0:
        drawn = block_scale(rng, shape, pieces, -0.22, 0.18) * drawn
    return jnp.clip(drawn, min=-most, max=most).astype(kind)


def setup_inputs(seed: int = 0) -> dict:
    key_of = jax.random.split(jax.random.key(seed), 11)
    return {
        "query_grads": draw_query_grads(jax.random.fold_in(key_of[10], 71), 0),
        "merge_grads": draw_merge_grads(jax.random.fold_in(key_of[10], 71), 0),
        "query_accum": draw_query_accum(jax.random.fold_in(key_of[10], 71), 0),
        "merge_accum": draw_merge_accum(jax.random.fold_in(key_of[10], 71), 0),
        "query_master": bell_draw(key_of[4], (LAYERS, D, QW), 0.05, 0.75, ((1, 16), (2, 16)), jnp.float32),
        "merge_master": bell_draw(key_of[5], (LAYERS, QW, D), 0.05, 0.75, ((1, 16), (2, 16)), jnp.float32),
        "query_moment": bell_draw(key_of[6], (LAYERS, D, QW), 1.0, 6.0, ((1, 16), (2, 16)), jnp.float32),
        "merge_moment": bell_draw(key_of[7], (LAYERS, QW, D), 1.0, 6.0, ((1, 16), (2, 16)), jnp.float32),
        "query_second": jnp.clip(jnp.exp(math.log(3.0) - 2.3025851 * jax.random.uniform(key_of[8], (LAYERS, D, QW), jnp.float32) ** block_scale(key_of[8], (LAYERS, D, QW), ((1, 16), (2, 16)), -0.2, 0.2)), 0.3, 3.0),
        "merge_second": jnp.clip(jnp.exp(math.log(3.0) - 2.3025851 * jax.random.uniform(key_of[9], (LAYERS, QW, D), jnp.float32) ** block_scale(key_of[9], (LAYERS, QW, D), ((1, 16), (2, 16)), -0.2, 0.2)), 0.3, 3.0),
    }


beta_one = 0.9
beta_two = 0.95
learn_rate = 0.002
weight_decay = 0.1
adam_eps = 1e-08

def adamw(total, clip, master, moment, second):
    scaled = clip * total
    first = beta_one * moment + (1.0 - beta_one) * scaled
    variance = beta_two * second + (1.0 - beta_two) * scaled * scaled
    corr_one = 1.0 - beta_one ** STEP
    corr_two = 1.0 - beta_two ** STEP
    update = first / corr_one / (jnp.sqrt(variance / corr_two) + adam_eps) + weight_decay * master
    return (master - learn_rate * update, first, variance)

def reference(query_grads, merge_grads, query_accum, merge_accum, query_master, merge_master, query_moment, merge_moment, query_second, merge_second):
    query_total = query_accum + lax.optimization_barrier(jnp.sum(query_grads.astype(jnp.float32), axis=0))
    merge_total = merge_accum + lax.optimization_barrier(jnp.sum(merge_grads.astype(jnp.float32), axis=0))
    sumsq = jnp.sum(query_total * query_total) + jnp.sum(merge_total * merge_total)
    clip = jnp.minimum(1.0, lax.rsqrt(sumsq / float(ENTRIES) + 1e-06))
    query_shard, query_first, query_variance = adamw(query_total, clip, query_master, query_moment, query_second)
    merge_shard, merge_first, merge_variance = adamw(merge_total, clip, merge_master, merge_moment, merge_second)
    return (query_shard.astype(jnp.bfloat16), merge_shard.astype(jnp.bfloat16), query_shard, merge_shard, query_first, merge_first, query_variance, merge_variance)
```

```python
import jax
import jax.numpy as jnp
from jax import lax
from jax.experimental import pallas as pl
from jax.experimental.pallas import tpu as pltpu
from jax.sharding import Mesh
from jax.sharding import PartitionSpec as P

STEP = 10
ENTRIES = 29360128
BETA_ONE = 0.9
BETA_TWO = 0.95
LEARN_RATE = 0.002
WEIGHT_DECAY = 0.1
ADAM_EPS = 1e-08

N = 4
ROWS = 224
COLS = 256
HALF = ROWS // 2
GROUP = N * ROWS
FULL = N * GROUP
BLOCK = 32
MESH_ID = pl.DeviceIdType.MESH
OFFSETS = (2, 1, 3, 0)

RELAY_A, RELAY_B, DIRECT_P, DIRECT_M, FORWARD_A, FORWARD_B = range(6)
T_A, T_B, U_P, U_M, V_P, V_M = range(6)


def wrap(value):
    return lax.rem(value, N)


def shard_rows(index, start=0, size=ROWS):
    return pl.ds(pl.multiple_of(index * ROWS + start, 16), size)


def kernel(
    grads_q, grads_m, accum_q, accum_m, master_q, master_m, moment_q, moment_m, second_q, second_m,
    weight_q, weight_m, shard_q, shard_m, first_q, first_m, variance_q, variance_m,
    raw_m, turned_m, own_q, held, relay, partial, t_buf, u_buf, v_buf, state, gather_m,
    plane_buf, column_buf, row_buf,
    load_sem, rs_send, rs_recv, second_send, second_recv, ag_send, ag_recv, ar_send, ar_recv,
):
    x, y = lax.axis_index("x"), lax.axis_index("y")
    z, c = lax.axis_index("z"), lax.axis_index("c")
    first_axis, second_axis = ("y", "x"), ("x", "y")
    f, s = (y, x), (x, y)

    def shard_index(a, fi, si):
        return si * N + fi if a == 0 else fi * N + si

    plane_peers, column_peers = [], []
    me_plane, me_column = x * N + y, z * 2 + c
    for d in range(1, 16):
        peer = lax.rem(me_plane + d, 16)
        plane_peers.append({"x": peer // N, "y": lax.rem(peer, N), "z": z, "c": c})
        peer = lax.rem(me_column + d, 16)
        column_peers.append({"x": x, "y": y, "z": peer // 2, "c": lax.rem(peer, 2)})

    def group_cols(fi):
        return pl.ds(pl.multiple_of(fi * GROUP, 128), GROUP)

    raw_loads = []
    for d in (2, 1, 3, 0):
        fi = wrap(x + d)
        copy = pltpu.make_async_copy(
            grads_m.at[:, group_cols(fi)], raw_m.at[:, group_cols(fi)], load_sem.at[d]
        )
        copy.start()
        raw_loads.append(copy)

    barrier = pltpu.get_barrier_semaphore()
    for peer in plane_peers + column_peers:
        pl.semaphore_signal(barrier, inc=1, device_id=peer, device_id_type=MESH_ID)

    own_loads = []
    for k in range(N):
        si = wrap(x + OFFSETS[k])
        copy = pltpu.make_async_copy(
            grads_q.at[shard_rows(si * N + y)], own_q.at[k], load_sem.at[4 + k]
        )
        copy.start()
        own_loads.append(copy)
    state_loads = []
    for i, ref in enumerate(
        (accum_q, accum_m, master_q, master_m, moment_q, moment_m, second_q, second_m)
    ):
        copy = pltpu.make_async_copy(ref, state.at[i], load_sem.at[8 + i])
        copy.start()
        state_loads.append(copy)

    pl.semaphore_wait(barrier, 30)

    def remote(src, dst, send, recv, axis, coordinate):
        return pltpu.make_async_remote_copy(
            src_ref=src,
            dst_ref=dst,
            send_sem=send,
            recv_sem=recv,
            device_id={axis: coordinate},
            device_id_type=MESH_ID,
        )

    started = []

    def go(copy):
        copy.start()
        started.append(copy)

    source = (grads_q, turned_m)

    def rs_copy(a, k, kind):
        fi, si = f[a], wrap(s[a] + OFFSETS[k])
        plus, minus, far = wrap(fi + 1), wrap(fi + 3), wrap(fi + 2)
        src = {
            RELAY_A: lambda: source[a].at[shard_rows(shard_index(a, far, si), 0, HALF)],
            RELAY_B: lambda: source[a].at[shard_rows(shard_index(a, far, si), HALF, HALF)],
            DIRECT_P: lambda: source[a].at[shard_rows(shard_index(a, plus, si))],
            DIRECT_M: lambda: source[a].at[shard_rows(shard_index(a, minus, si))],
            FORWARD_A: lambda: relay.at[a, k, 0],
            FORWARD_B: lambda: relay.at[a, k, 1],
        }[kind]()
        dst = {
            RELAY_A: lambda: relay.at[a, k, 0],
            RELAY_B: lambda: relay.at[a, k, 1],
            DIRECT_P: lambda: held.at[a, k, 0],
            DIRECT_M: lambda: held.at[a, k, 1],
            FORWARD_A: lambda: held.at[a, k, 2, pl.ds(0, HALF)],
            FORWARD_B: lambda: held.at[a, k, 2, pl.ds(HALF, HALF)],
        }[kind]()
        target = plus if kind in (RELAY_A, DIRECT_P, FORWARD_A) else minus
        return remote(
            src, dst, rs_send.at[a, k, kind], rs_recv.at[a, k, kind], first_axis[a], target
        )

    def raw_relay(a, k):
        go(rs_copy(a, k, RELAY_A))
        go(rs_copy(a, k, RELAY_B))

    def raw_direct(a, k):
        go(rs_copy(a, k, DIRECT_P))
        go(rs_copy(a, k, DIRECT_M))

    def forward(a, k):
        rs_copy(a, k, RELAY_A).wait_recv()
        go(rs_copy(a, k, FORWARD_A))
        rs_copy(a, k, RELAY_B).wait_recv()
        go(rs_copy(a, k, FORWARD_B))

    def turn(fi):
        def step(i, carry):
            at = pl.ds(pl.multiple_of(fi * GROUP + i * 128, 128), 128)
            turned_m[at, :] = raw_m[:, at].T
            return carry

        lax.fori_loop(0, GROUP // 128, step, 0)

    def add_up(a, k):
        for kind in (DIRECT_P, DIRECT_M, FORWARD_A, FORWARD_B):
            rs_copy(a, k, kind).wait_recv()
        if a == 0:
            own_loads[k].wait()
        if k == 3:
            state_loads[a].wait()
        own_base = 0 if a == 0 else shard_index(a, f[a], wrap(s[a] + OFFSETS[k])) * ROWS

        def step(i, carry):
            at = pl.ds(pl.multiple_of(i * BLOCK, BLOCK), BLOCK)
            if a == 0:
                mine = own_q[k, at, :]
            else:
                mine = turned_m[pl.ds(pl.multiple_of(own_base + i * BLOCK, BLOCK), BLOCK), :]
            value = mine.astype(jnp.float32)
            for j in range(3):
                value = value + held[a, k, j, at, :].astype(jnp.float32)
            if k == 3:
                value = value + state[a, at, :]
            partial[a, k, at, :] = value
            return carry

        lax.fori_loop(0, ROWS // BLOCK, step, 0)

    low, high = pl.ds(0, HALF), pl.ds(HALF, HALF)

    def second_copy(a, kind):
        plus, minus = wrap(s[a] + 1), wrap(s[a] + 3)
        src, dst, target = {
            T_A: (partial.at[a, 0, low], t_buf.at[a, 0], plus),
            T_B: (partial.at[a, 0, high], t_buf.at[a, 1], minus),
            U_P: (partial.at[a, 1, high], u_buf.at[a, 0], plus),
            U_M: (partial.at[a, 2, low], u_buf.at[a, 1], minus),
            V_P: (partial.at[a, 1, low], v_buf.at[a, 0], plus),
            V_M: (partial.at[a, 2, high], v_buf.at[a, 1], minus),
        }[kind]
        return remote(
            src, dst, second_send.at[a, kind], second_recv.at[a, kind], second_axis[a], target
        )

    def merge_t(a):
        second_copy(a, T_A).wait_recv()
        partial[a, 1, 0:HALF, :] = partial[a, 1, 0:HALF, :] + t_buf[a, 0]
        go(second_copy(a, V_P))
        second_copy(a, T_B).wait_recv()
        partial[a, 2, HALF:ROWS, :] = partial[a, 2, HALF:ROWS, :] + t_buf[a, 1]
        go(second_copy(a, V_M))

    def squares(value):
        return jnp.sum((value * value).reshape(-1, 8, COLS), axis=0)

    def finish(a, acc):
        for kind in (U_P, U_M, V_P, V_M):
            second_copy(a, kind).wait_recv()
        for h, one, two in ((0, v_buf, u_buf), (1, u_buf, v_buf)):
            def step(i, acc):
                at = pl.ds(pl.multiple_of(i * 16, 16), 16)
                here = pl.ds(pl.multiple_of(h * HALF + i * 16, 16), 16)
                total = partial[a, 3, here, :] + one[a, 0, at, :] + two[a, 1, at, :]
                partial[a, 3, here, :] = total
                return acc + squares(total)

            acc = lax.fori_loop(0, HALF // 16, step, acc)
        return acc

    raw_relay(0, 0)
    raw_direct(0, 0)
    raw_relay(0, 1)
    raw_direct(0, 1)
    raw_loads[0].wait()
    turn(wrap(x + 2))
    raw_relay(1, 0)
    raw_loads[1].wait()
    turn(wrap(x + 1))
    go(rs_copy(1, 0, DIRECT_P))
    raw_loads[2].wait()
    turn(wrap(x + 3))
    go(rs_copy(1, 0, DIRECT_M))
    raw_relay(1, 1)
    raw_direct(1, 1)
    raw_loads[3].wait()
    turn(x)
    for k in (0, 1):
        for a in (0, 1):
            forward(a, k)
            raw_relay(a, k + 2)
            raw_direct(a, k + 2)
    for a in (0, 1):
        forward(a, 2)
        add_up(a, 0)
        go(second_copy(a, T_A))
        go(second_copy(a, T_B))
    for a in (0, 1):
        forward(a, 3)
        add_up(a, 1)
        go(second_copy(a, U_P))
    for a in (0, 1):
        add_up(a, 2)
        go(second_copy(a, U_M))
    for a in (0, 1):
        merge_t(a)
    for a in (0, 1):
        add_up(a, 3)
    acc = jnp.zeros((8, COLS), jnp.float32)
    for a in (0, 1):
        acc = finish(a, acc)

    def exchange(stage, row, buf, me, peers):
        row_buf[stage] = row
        buf[me] = row
        for d, peer in enumerate(peers):
            copy = pltpu.make_async_remote_copy(
                src_ref=row_buf.at[stage],
                dst_ref=buf.at[me],
                send_sem=ar_send.at[stage, d],
                recv_sem=ar_recv.at[stage, d],
                device_id=peer,
                device_id_type=MESH_ID,
            )
            go(copy)
        for d in range(15):
            sender = lax.rem(me + 15 - d, 16)
            pltpu.make_async_remote_copy(
                src_ref=row_buf.at[stage],
                dst_ref=buf.at[sender],
                send_sem=ar_send.at[stage, d],
                recv_sem=ar_recv.at[stage, d],
                device_id=peers[d],
                device_id_type=MESH_ID,
            ).wait_recv()
        return jnp.sum(buf[...], axis=0)

    row = jnp.sum(acc, axis=0, keepdims=True)
    row = row[:, :128] + row[:, 128:]
    row = exchange(0, row, plane_buf, me_plane, plane_peers)
    row = exchange(1, row, column_buf, me_column, column_peers)
    sumsq = jnp.sum(row, axis=1, keepdims=True)
    clip = jnp.minimum(1.0, lax.rsqrt(sumsq / float(ENTRIES) + 1e-06))

    gathered = (weight_q, gather_m)
    outs = ((shard_q, first_q, variance_q), (shard_m, first_m, variance_m))
    for copy in state_loads[2:]:
        copy.wait()

    def update(a):
        base = shard_index(a, f[a], s[a]) * ROWS
        shard_out, first_out, variance_out = outs[a]

        def step(i, carry):
            at = pl.ds(pl.multiple_of(i * BLOCK, BLOCK), BLOCK)
            scaled = clip * partial[a, 3, at, :]
            master = state[2 + a, at, :]
            first = BETA_ONE * state[4 + a, at, :] + (1.0 - BETA_ONE) * scaled
            variance = BETA_TWO * state[6 + a, at, :] + (1.0 - BETA_TWO) * scaled * scaled
            corr_one = 1.0 - BETA_ONE**STEP
            corr_two = 1.0 - BETA_TWO**STEP
            change = (
                first / corr_one / (jnp.sqrt(variance / corr_two) + ADAM_EPS)
                + WEIGHT_DECAY * master
            )
            shard = master - LEARN_RATE * change
            shard_out[at, :] = shard
            first_out[at, :] = first
            variance_out[at, :] = variance
            gathered[a][pl.ds(pl.multiple_of(base + i * BLOCK, BLOCK), BLOCK), :] = shard.astype(
                jnp.bfloat16
            )
            return carry

        lax.fori_loop(0, ROWS // BLOCK, step, 0)

    ITEMS = (0, 3, 1, 2)

    def ag_copy(a, item, kind):
        if item == 0:
            axis, here = second_axis[a], s[a]
        else:
            axis, here = first_axis[a], f[a]
        owner = {0: here, 1: here, 2: wrap(here + 3), 3: wrap(here + 1)}[kind]
        if item == 0:
            index = shard_index(a, f[a], owner)
        else:
            index = shard_index(a, owner, wrap(s[a] + ITEMS[item - 1]))
        start, size = {0: (0, ROWS), 1: (0, ROWS), 2: (0, HALF), 3: (HALF, HALF)}[kind]
        ref = gathered[a].at[shard_rows(index, start, size)]
        target = wrap(here + 1) if kind in (0, 2) else wrap(here + 3)
        return remote(ref, ref, ag_send.at[a, item, kind], ag_recv.at[a, item, kind], axis, target)

    def ag_wait(a, item, kind):
        if item == 0:
            axis, here = second_axis[a], s[a]
        else:
            axis, here = first_axis[a], f[a]
        owner = {0: wrap(here + 3), 1: wrap(here + 1), 2: wrap(here + 2), 3: wrap(here + 2)}[kind]
        if item == 0:
            index = shard_index(a, f[a], owner)
        else:
            index = shard_index(a, owner, wrap(s[a] + ITEMS[item - 1]))
        start, size = {0: (0, ROWS), 1: (0, ROWS), 2: (0, HALF), 3: (HALF, HALF)}[kind]
        ref = gathered[a].at[shard_rows(index, start, size)]
        remote(
            ref, ref, ag_send.at[a, item, kind], ag_recv.at[a, item, kind], axis, here
        ).wait_recv()

    def turn_back(fi):
        def step(i, carry):
            at = pl.ds(pl.multiple_of(fi * GROUP + i * 128, 128), 128)
            weight_m[:, at] = gather_m[at, :].T
            return carry

        lax.fori_loop(0, GROUP // 128, step, 0)

    for a in (0, 1):
        update(a)
        for item in (0, 1):
            go(ag_copy(a, item, 0))
            go(ag_copy(a, item, 1))
    for a in (0, 1):
        ag_wait(a, 0, 0)
        go(ag_copy(a, 0, 2))
        ag_wait(a, 0, 1)
        go(ag_copy(a, 0, 3))
        for item in (2, 3):
            go(ag_copy(a, item, 0))
            go(ag_copy(a, item, 1))

    def ag_forward(a, item):
        ag_wait(a, item, 0)
        go(ag_copy(a, item, 2))
        ag_wait(a, item, 1)
        go(ag_copy(a, item, 3))

    for a in (0, 1):
        ag_forward(a, 1)
    for a in (0, 1):
        ag_wait(a, 0, 2)
        ag_wait(a, 0, 3)
        go(ag_copy(a, 4, 0))
        go(ag_copy(a, 4, 1))
    turn_back(x)
    for item in (2, 3, 4):
        for a in (0, 1):
            ag_forward(a, item)
    turn_back(wrap(x + 1))
    turn_back(wrap(x + 3))
    for item in (1, 2, 3, 4):
        for a in (0, 1):
            ag_wait(a, item, 2)
            ag_wait(a, item, 3)
    turn_back(wrap(x + 2))
    for copy in started:
        copy.wait_send()


def on_device(
    query_grads, merge_grads, query_accum, merge_accum, query_master, merge_master,
    query_moment, merge_moment, query_second, merge_second,
):
    def flat(value):
        return value.reshape(ROWS, COLS)

    def turned(value):
        return jnp.swapaxes(value[0], 0, 1)

    bf16, f32 = jnp.bfloat16, jnp.float32
    any_spec = pl.BlockSpec(memory_space=pl.ANY)
    shard = pltpu.VMEM((ROWS, COLS), f32)
    outs = pl.pallas_call(
        kernel,
        name="adamw_step",
        out_shape=[
            pltpu.VMEM((FULL, COLS), bf16),
            pltpu.VMEM((COLS, FULL), bf16),
            shard, shard, shard, shard, shard, shard,
        ],
        in_specs=[any_spec] * 10,
        out_specs=[pl.BlockSpec(memory_space=pltpu.VMEM)] * 8,
        scratch_shapes=[
            pltpu.VMEM((COLS, FULL), bf16),
            pltpu.VMEM((FULL, COLS), bf16),
            pltpu.VMEM((N, ROWS, COLS), bf16),
            pltpu.VMEM((2, N, 3, ROWS, COLS), bf16),
            pltpu.VMEM((2, N, 2, HALF, COLS), bf16),
            pltpu.VMEM((2, N, ROWS, COLS), f32),
            pltpu.VMEM((2, 2, HALF, COLS), f32),
            pltpu.VMEM((2, 2, HALF, COLS), f32),
            pltpu.VMEM((2, 2, HALF, COLS), f32),
            pltpu.VMEM((8, ROWS, COLS), f32),
            pltpu.VMEM((FULL, COLS), bf16),
            pltpu.VMEM((16, 1, 128), f32),
            pltpu.VMEM((16, 1, 128), f32),
            pltpu.VMEM((2, 1, 128), f32),
            pltpu.SemaphoreType.DMA((16,)),
            pltpu.SemaphoreType.DMA((2, N, 6)),
            pltpu.SemaphoreType.DMA((2, N, 6)),
            pltpu.SemaphoreType.DMA((2, 6)),
            pltpu.SemaphoreType.DMA((2, 6)),
            pltpu.SemaphoreType.DMA((2, 5, 4)),
            pltpu.SemaphoreType.DMA((2, 5, 4)),
            pltpu.SemaphoreType.DMA((2, 15)),
            pltpu.SemaphoreType.DMA((2, 15)),
        ],
        compiler_params=pltpu.CompilerParams(
            collective_id=0, has_side_effects=True, vmem_limit_bytes=32 * 2**20
        ),
    )(
        query_grads.reshape(FULL, COLS), merge_grads.reshape(COLS, FULL),
        flat(query_accum), turned(merge_accum), flat(query_master), turned(merge_master),
        flat(query_moment), turned(merge_moment), flat(query_second), turned(merge_second),
    )
    weight_q, weight_m, shard_q, shard_m, first_q, first_m, variance_q, variance_m = outs

    def back(value):
        return jnp.swapaxes(value, 0, 1)[None]

    return (
        weight_q[None], weight_m[None],
        shard_q[None], back(shard_m), first_q[None], back(first_m), variance_q[None], back(variance_m),
    )


def solution(mesh):
    finer = Mesh(mesh.devices.reshape(4, 4, 8, 2), ("x", "y", "z", "c"))
    dp, mp = ("x", "y"), ("z", "c")
    query, merge = P(None, dp, mp), P(None, mp, dp)
    return jax.shard_map(
        on_device,
        mesh=finer,
        in_specs=(P(dp, None, None, mp), P(dp, None, mp, None)) + (query, merge) * 4,
        out_specs=(P(None, None, mp), P(None, mp, None)) + (query, merge) * 3,
        check_vma=False,
    )
```

```python
import jax
import jax.numpy as jnp
from jax import lax
from jax.experimental import pallas as pl
from jax.experimental.pallas import tpu as pltpu
from jax.sharding import Mesh
from jax.sharding import PartitionSpec as P

STEP = 10
ENTRIES = 29360128
BETA_ONE = 0.9
BETA_TWO = 0.95
LEARN_RATE = 0.002
WEIGHT_DECAY = 0.1
ADAM_EPS = 1e-08

N = 4
ROWS = 224
COLS = 256
HALF = ROWS // 2
GROUP = N * ROWS
FULL = N * GROUP
BLOCK = 32
MESH_ID = pl.DeviceIdType.MESH
OFFSETS = (2, 1, 3, 0)

RELAY_A, RELAY_B, DIRECT_P, DIRECT_M, FORWARD_A, FORWARD_B = range(6)
T_A, T_B, U_P, U_M, V_P, V_M = range(6)


def wrap(value):
    return lax.rem(value, N)


def shard_rows(index, start=0, size=ROWS):
    return pl.ds(pl.multiple_of(index * ROWS + start, 16), size)


def kernel(
    grads_q, grads_m, accum_q, accum_m, master_q, master_m, moment_q, moment_m, second_q, second_m,
    weight_q, weight_m, shard_q, shard_m, first_q, first_m, variance_q, variance_m,
    raw_m, turned_m, own_q, held, relay, partial, t_buf, u_buf, v_buf, state, gather_m,
    plane_buf, column_buf, row_buf,
    load_sem, rs_send, rs_recv, second_send, second_recv, ag_send, ag_recv, ar_send, ar_recv,
):
    x, y = lax.axis_index("x"), lax.axis_index("y")
    z, c = lax.axis_index("z"), lax.axis_index("c")
    first_axis, second_axis = ("y", "x"), ("x", "y")
    f, s = (y, x), (x, y)

    def shard_index(a, fi, si):
        return si * N + fi if a == 0 else fi * N + si

    plane_peers, column_peers = [], []
    me_plane, me_column = x * N + y, z * 2 + c
    for d in range(1, 16):
        peer = lax.rem(me_plane + d, 16)
        plane_peers.append({"x": peer // N, "y": lax.rem(peer, N), "z": z, "c": c})
        peer = lax.rem(me_column + d, 16)
        column_peers.append({"x": x, "y": y, "z": peer // 2, "c": lax.rem(peer, 2)})

    def group_cols(fi):
        return pl.ds(pl.multiple_of(fi * GROUP, 128), GROUP)

    raw_loads = []
    for d in (2, 1, 3, 0):
        fi = wrap(x + d)
        copy = pltpu.make_async_copy(
            grads_m.at[:, group_cols(fi)], raw_m.at[:, group_cols(fi)], load_sem.at[d]
        )
        copy.start()
        raw_loads.append(copy)

    barrier = pltpu.get_barrier_semaphore()
    for peer in plane_peers + column_peers:
        pl.semaphore_signal(barrier, inc=1, device_id=peer, device_id_type=MESH_ID)

    own_loads = []
    for k in range(N):
        si = wrap(x + OFFSETS[k])
        copy = pltpu.make_async_copy(
            grads_q.at[shard_rows(si * N + y)], own_q.at[k], load_sem.at[4 + k]
        )
        copy.start()
        own_loads.append(copy)
    state_loads = []
    for i, ref in enumerate(
        (accum_q, accum_m, master_q, master_m, moment_q, moment_m, second_q, second_m)
    ):
        copy = pltpu.make_async_copy(ref, state.at[i], load_sem.at[8 + i])
        copy.start()
        state_loads.append(copy)

    pl.semaphore_wait(barrier, 30)

    def remote(src, dst, send, recv, axis, coordinate):
        return pltpu.make_async_remote_copy(
            src_ref=src,
            dst_ref=dst,
            send_sem=send,
            recv_sem=recv,
            device_id={axis: coordinate},
            device_id_type=MESH_ID,
        )

    started = []

    def go(copy):
        copy.start()
        started.append(copy)

    source = (grads_q, turned_m)

    def rs_copy(a, k, kind):
        fi, si = f[a], wrap(s[a] + OFFSETS[k])
        plus, minus, far = wrap(fi + 1), wrap(fi + 3), wrap(fi + 2)
        src = {
            RELAY_A: lambda: source[a].at[shard_rows(shard_index(a, far, si), 0, HALF)],
            RELAY_B: lambda: source[a].at[shard_rows(shard_index(a, far, si), HALF, HALF)],
            DIRECT_P: lambda: source[a].at[shard_rows(shard_index(a, plus, si))],
            DIRECT_M: lambda: source[a].at[shard_rows(shard_index(a, minus, si))],
            FORWARD_A: lambda: relay.at[a, k, 0],
            FORWARD_B: lambda: relay.at[a, k, 1],
        }[kind]()
        dst = {
            RELAY_A: lambda: relay.at[a, k, 0],
            RELAY_B: lambda: relay.at[a, k, 1],
            DIRECT_P: lambda: held.at[a, k, 0],
            DIRECT_M: lambda: held.at[a, k, 1],
            FORWARD_A: lambda: held.at[a, k, 2, pl.ds(0, HALF)],
            FORWARD_B: lambda: held.at[a, k, 2, pl.ds(HALF, HALF)],
        }[kind]()
        target = plus if kind in (RELAY_A, DIRECT_P, FORWARD_A) else minus
        return remote(
            src, dst, rs_send.at[a, k, kind], rs_recv.at[a, k, kind], first_axis[a], target
        )

    def raw_relay(a, k):
        go(rs_copy(a, k, RELAY_A))
        go(rs_copy(a, k, RELAY_B))

    def raw_direct(a, k):
        go(rs_copy(a, k, DIRECT_P))
        go(rs_copy(a, k, DIRECT_M))

    def forward(a, k):
        rs_copy(a, k, RELAY_A).wait_recv()
        go(rs_copy(a, k, FORWARD_A))
        rs_copy(a, k, RELAY_B).wait_recv()
        go(rs_copy(a, k, FORWARD_B))

    def turn(fi):
        def step(i, carry):
            at = pl.ds(pl.multiple_of(fi * GROUP + i * 128, 128), 128)
            turned_m[at, :] = raw_m[:, at].T
            return carry

        lax.fori_loop(0, GROUP // 128, step, 0)

    def add_up(a, k):
        for kind in (DIRECT_P, DIRECT_M, FORWARD_A, FORWARD_B):
            rs_copy(a, k, kind).wait_recv()
        if a == 0:
            own_loads[k].wait()
        if k == 3:
            state_loads[a].wait()
        own_base = 0 if a == 0 else shard_index(a, f[a], wrap(s[a] + OFFSETS[k])) * ROWS

        def step(i, carry):
            at = pl.ds(pl.multiple_of(i * BLOCK, BLOCK), BLOCK)
            if a == 0:
                mine = own_q[k, at, :]
            else:
                mine = turned_m[pl.ds(pl.multiple_of(own_base + i * BLOCK, BLOCK), BLOCK), :]
            value = mine.astype(jnp.float32)
            for j in range(3):
                value = value + held[a, k, j, at, :].astype(jnp.float32)
            if k == 3:
                value = value + state[a, at, :]
            partial[a, k, at, :] = value
            return carry

        lax.fori_loop(0, ROWS // BLOCK, step, 0)

    low, high = pl.ds(0, HALF), pl.ds(HALF, HALF)

    def second_copy(a, kind):
        plus, minus = wrap(s[a] + 1), wrap(s[a] + 3)
        src, dst, target = {
            T_A: (partial.at[a, 0, low], t_buf.at[a, 0], plus),
            T_B: (partial.at[a, 0, high], t_buf.at[a, 1], minus),
            U_P: (partial.at[a, 1, high], u_buf.at[a, 0], plus),
            U_M: (partial.at[a, 2, low], u_buf.at[a, 1], minus),
            V_P: (partial.at[a, 1, low], v_buf.at[a, 0], plus),
            V_M: (partial.at[a, 2, high], v_buf.at[a, 1], minus),
        }[kind]
        return remote(
            src, dst, second_send.at[a, kind], second_recv.at[a, kind], second_axis[a], target
        )

    def merge_t(a):
        second_copy(a, T_A).wait_recv()
        partial[a, 1, 0:HALF, :] = partial[a, 1, 0:HALF, :] + t_buf[a, 0]
        go(second_copy(a, V_P))
        second_copy(a, T_B).wait_recv()
        partial[a, 2, HALF:ROWS, :] = partial[a, 2, HALF:ROWS, :] + t_buf[a, 1]
        go(second_copy(a, V_M))

    def squares(value):
        return jnp.sum((value * value).reshape(-1, 8, COLS), axis=0)

    def finish(a, acc):
        for kind in (U_P, U_M, V_P, V_M):
            second_copy(a, kind).wait_recv()
        for h, one, two in ((0, v_buf, u_buf), (1, u_buf, v_buf)):
            def step(i, acc):
                at = pl.ds(pl.multiple_of(i * 16, 16), 16)
                here = pl.ds(pl.multiple_of(h * HALF + i * 16, 16), 16)
                total = partial[a, 3, here, :] + one[a, 0, at, :] + two[a, 1, at, :]
                partial[a, 3, here, :] = total
                return acc + squares(total)

            acc = lax.fori_loop(0, HALF // 16, step, acc)
        return acc

    raw_relay(0, 0)
    raw_direct(0, 0)
    raw_relay(0, 1)
    raw_direct(0, 1)
    raw_loads[0].wait()
    turn(wrap(x + 2))
    raw_relay(1, 0)
    raw_loads[1].wait()
    turn(wrap(x + 1))
    go(rs_copy(1, 0, DIRECT_P))
    raw_loads[2].wait()
    turn(wrap(x + 3))
    go(rs_copy(1, 0, DIRECT_M))
    raw_relay(1, 1)
    raw_direct(1, 1)
    raw_loads[3].wait()
    turn(x)
    for k in (0, 1):
        for a in (0, 1):
            forward(a, k)
            raw_relay(a, k + 2)
            raw_direct(a, k + 2)
    for a in (0, 1):
        forward(a, 2)
        add_up(a, 0)
        go(second_copy(a, T_A))
        go(second_copy(a, T_B))
    for a in (0, 1):
        forward(a, 3)
        add_up(a, 1)
        go(second_copy(a, U_P))
    for a in (0, 1):
        add_up(a, 2)
        go(second_copy(a, U_M))
    for a in (0, 1):
        merge_t(a)
    for a in (0, 1):
        add_up(a, 3)
    acc = jnp.zeros((8, COLS), jnp.float32)
    for a in (0, 1):
        acc = finish(a, acc)

    def exchange(stage, row, buf, me, peers):
        row_buf[stage] = row
        buf[me] = row
        for d, peer in enumerate(peers):
            copy = pltpu.make_async_remote_copy(
                src_ref=row_buf.at[stage],
                dst_ref=buf.at[me],
                send_sem=ar_send.at[stage, d],
                recv_sem=ar_recv.at[stage, d],
                device_id=peer,
                device_id_type=MESH_ID,
            )
            go(copy)
        for d in range(15):
            sender = lax.rem(me + 15 - d, 16)
            pltpu.make_async_remote_copy(
                src_ref=row_buf.at[stage],
                dst_ref=buf.at[sender],
                send_sem=ar_send.at[stage, d],
                recv_sem=ar_recv.at[stage, d],
                device_id=peers[d],
                device_id_type=MESH_ID,
            ).wait_recv()
        return jnp.sum(buf[...], axis=0)

    row = jnp.sum(acc, axis=0, keepdims=True)
    row = row[:, :128] + row[:, 128:]
    row = exchange(0, row, plane_buf, me_plane, plane_peers)
    row = exchange(1, row, column_buf, me_column, column_peers)
    sumsq = jnp.sum(row, axis=1, keepdims=True)
    clip = jnp.minimum(1.0, lax.rsqrt(sumsq / float(ENTRIES) + 1e-06))

    gathered = (weight_q, gather_m)
    outs = ((shard_q, first_q, variance_q), (shard_m, first_m, variance_m))
    for copy in state_loads[2:]:
        copy.wait()

    def update(a):
        base = shard_index(a, f[a], s[a]) * ROWS
        shard_out, first_out, variance_out = outs[a]

        def step(i, carry):
            at = pl.ds(pl.multiple_of(i * BLOCK, BLOCK), BLOCK)
            scaled = clip * partial[a, 3, at, :]
            master = state[2 + a, at, :]
            first = BETA_ONE * state[4 + a, at, :] + (1.0 - BETA_ONE) * scaled
            variance = BETA_TWO * state[6 + a, at, :] + (1.0 - BETA_TWO) * scaled * scaled
            corr_one = 1.0 - BETA_ONE**STEP
            corr_two = 1.0 - BETA_TWO**STEP
            change = (
                first / corr_one / (jnp.sqrt(variance / corr_two) + ADAM_EPS)
                + WEIGHT_DECAY * master
            )
            shard = master - LEARN_RATE * change
            shard_out[at, :] = shard
            first_out[at, :] = first
            variance_out[at, :] = variance
            gathered[a][pl.ds(pl.multiple_of(base + i * BLOCK, BLOCK), BLOCK), :] = shard.astype(
                jnp.bfloat16
            )
            return carry

        lax.fori_loop(0, ROWS // BLOCK, step, 0)

    ITEMS = (0, 3, 1, 2)

    def ag_copy(a, item, kind):
        if item == 0:
            axis, here = second_axis[a], s[a]
        else:
            axis, here = first_axis[a], f[a]
        owner = {0: here, 1: here, 2: wrap(here + 3), 3: wrap(here + 1)}[kind]
        if item == 0:
            index = shard_index(a, f[a], owner)
        else:
            index = shard_index(a, owner, wrap(s[a] + ITEMS[item - 1]))
        start, size = {0: (0, ROWS), 1: (0, ROWS), 2: (0, HALF), 3: (HALF, HALF)}[kind]
        ref = gathered[a].at[shard_rows(index, start, size)]
        target = wrap(here + 1) if kind in (0, 2) else wrap(here + 3)
        return remote(ref, ref, ag_send.at[a, item, kind], ag_recv.at[a, item, kind], axis, target)

    def ag_wait(a, item, kind):
        if item == 0:
            axis, here = second_axis[a], s[a]
        else:
            axis, here = first_axis[a], f[a]
        owner = {0: wrap(here + 3), 1: wrap(here + 1), 2: wrap(here + 2), 3: wrap(here + 2)}[kind]
        if item == 0:
            index = shard_index(a, f[a], owner)
        else:
            index = shard_index(a, owner, wrap(s[a] + ITEMS[item - 1]))
        start, size = {0: (0, ROWS), 1: (0, ROWS), 2: (0, HALF), 3: (HALF, HALF)}[kind]
        ref = gathered[a].at[shard_rows(index, start, size)]
        remote(
            ref, ref, ag_send.at[a, item, kind], ag_recv.at[a, item, kind], axis, here
        ).wait_recv()

    def turn_back(fi):
        def step(i, carry):
            at = pl.ds(pl.multiple_of(fi * GROUP + i * 128, 128), 128)
            weight_m[:, at] = gather_m[at, :].T
            return carry

        lax.fori_loop(0, GROUP // 128, step, 0)

    for a in (0, 1):
        update(a)
        for item in (0, 1):
            go(ag_copy(a, item, 0))
            go(ag_copy(a, item, 1))
    for a in (0, 1):
        ag_wait(a, 0, 0)
        go(ag_copy(a, 0, 2))
        ag_wait(a, 0, 1)
        go(ag_copy(a, 0, 3))
        for item in (2, 3):
            go(ag_copy(a, item, 0))
            go(ag_copy(a, item, 1))

    def ag_forward(a, item):
        ag_wait(a, item, 0)
        go(ag_copy(a, item, 2))
        ag_wait(a, item, 1)
        go(ag_copy(a, item, 3))

    for a in (0, 1):
        ag_forward(a, 1)
    for a in (0, 1):
        ag_wait(a, 0, 2)
        ag_wait(a, 0, 3)
        go(ag_copy(a, 4, 0))
        go(ag_copy(a, 4, 1))
    turn_back(x)
    for item in (2, 3, 4):
        for a in (0, 1):
            ag_forward(a, item)
    turn_back(wrap(x + 1))
    turn_back(wrap(x + 3))
    for item in (1, 2, 3, 4):
        for a in (0, 1):
            ag_wait(a, item, 2)
            ag_wait(a, item, 3)
    turn_back(wrap(x + 2))
    for copy in started:
        copy.wait_send()


def write_out(*refs):
    sources, targets, sem = refs[:8], refs[8:16], refs[16]
    copies = [
        pltpu.make_async_copy(source, target, sem.at[i])
        for i, (source, target) in enumerate(zip(sources, targets))
    ]
    for copy in copies:
        copy.start()
    for copy in copies:
        copy.wait()


def on_device(
    query_grads, merge_grads, query_accum, merge_accum, query_master, merge_master,
    query_moment, merge_moment, query_second, merge_second,
):
    def flat(value):
        return value.reshape(ROWS, COLS)

    def turned(value):
        return jnp.swapaxes(value[0], 0, 1)

    bf16, f32 = jnp.bfloat16, jnp.float32
    hbm_spec = pl.BlockSpec(memory_space=pltpu.HBM)
    shard = pltpu.VMEM((ROWS, COLS), f32)
    operands = (
        query_grads.reshape(FULL, COLS), merge_grads.reshape(COLS, FULL),
        flat(query_accum), turned(merge_accum), flat(query_master), turned(merge_master),
        flat(query_moment), turned(merge_moment), flat(query_second), turned(merge_second),
    )
    operands = [pltpu.with_memory_space_constraint(value, pltpu.HBM) for value in operands]
    outs = pl.pallas_call(
        kernel,
        name="adamw_step",
        out_shape=[
            pltpu.VMEM((FULL, COLS), bf16),
            pltpu.VMEM((COLS, FULL), bf16),
            shard, shard, shard, shard, shard, shard,
        ],
        in_specs=[hbm_spec] * 10,
        out_specs=[pl.BlockSpec(memory_space=pltpu.VMEM)] * 8,
        scratch_shapes=[
            pltpu.VMEM((COLS, FULL), bf16),
            pltpu.VMEM((FULL, COLS), bf16),
            pltpu.VMEM((N, ROWS, COLS), bf16),
            pltpu.VMEM((2, N, 3, ROWS, COLS), bf16),
            pltpu.VMEM((2, N, 2, HALF, COLS), bf16),
            pltpu.VMEM((2, N, ROWS, COLS), f32),
            pltpu.VMEM((2, 2, HALF, COLS), f32),
            pltpu.VMEM((2, 2, HALF, COLS), f32),
            pltpu.VMEM((2, 2, HALF, COLS), f32),
            pltpu.VMEM((8, ROWS, COLS), f32),
            pltpu.VMEM((FULL, COLS), bf16),
            pltpu.VMEM((16, 1, 128), f32),
            pltpu.VMEM((16, 1, 128), f32),
            pltpu.VMEM((2, 1, 128), f32),
            pltpu.SemaphoreType.DMA((16,)),
            pltpu.SemaphoreType.DMA((2, N, 6)),
            pltpu.SemaphoreType.DMA((2, N, 6)),
            pltpu.SemaphoreType.DMA((2, 6)),
            pltpu.SemaphoreType.DMA((2, 6)),
            pltpu.SemaphoreType.DMA((2, 5, 4)),
            pltpu.SemaphoreType.DMA((2, 5, 4)),
            pltpu.SemaphoreType.DMA((2, 15)),
            pltpu.SemaphoreType.DMA((2, 15)),
        ],
        compiler_params=pltpu.CompilerParams(
            collective_id=0, has_side_effects=True, vmem_limit_bytes=32 * 2**20
        ),
    )(*operands)
    outs = pl.pallas_call(
        write_out,
        name="write_out",
        out_shape=[jax.ShapeDtypeStruct(out.shape, out.dtype) for out in outs],
        in_specs=[pl.BlockSpec(memory_space=pltpu.VMEM)] * 8,
        out_specs=[hbm_spec] * 8,
        scratch_shapes=[pltpu.SemaphoreType.DMA((8,))],
        compiler_params=pltpu.CompilerParams(vmem_limit_bytes=2**20),
    )(*outs)
    weight_q, weight_m, shard_q, shard_m, first_q, first_m, variance_q, variance_m = outs

    def back(value):
        return jnp.swapaxes(value, 0, 1)[None]

    return (
        weight_q[None], weight_m[None],
        shard_q[None], back(shard_m), first_q[None], back(first_m), variance_q[None], back(variance_m),
    )


def solution(mesh):
    finer = Mesh(mesh.devices.reshape(4, 4, 8, 2), ("x", "y", "z", "c"))
    dp, mp = ("x", "y"), ("z", "c")
    query, merge = P(None, dp, mp), P(None, mp, dp)
    return jax.shard_map(
        on_device,
        mesh=finer,
        in_specs=(P(dp, None, None, mp), P(dp, None, mp, None)) + (query, merge) * 4,
        out_specs=(P(None, None, mp), P(None, mp, None)) + (query, merge) * 3,
        check_vma=False,
    )
```

```python
import jax
import jax.numpy as jnp
from jax import lax
from jax.experimental import pallas as pl
from jax.experimental.pallas import tpu as pltpu
from jax.sharding import Mesh
from jax.sharding import PartitionSpec as P

STEP = 10
ENTRIES = 29360128
BETA_ONE = 0.9
BETA_TWO = 0.95
LEARN_RATE = 0.002
WEIGHT_DECAY = 0.1
ADAM_EPS = 1e-08

N = 4
ROWS = 224
COLS = 256
HALF = ROWS // 2
GROUP = N * ROWS
FULL = N * GROUP
BLOCK = 32
MESH_ID = pl.DeviceIdType.MESH
OFFSETS = (2, 1, 3, 0)

RELAY_A, RELAY_B, RAW_P, RAW_M, SUM_P, SUM_M = range(6)
T_A, T_B, U_P, U_M, V_P, V_M = range(6)


def wrap(value):
    return lax.rem(value, N)


def shard_rows(index, start=0, size=ROWS):
    return pl.ds(pl.multiple_of(index * ROWS + start, 16), size)


def kernel(
    grads_q, grads_m, accum_q, accum_m, master_q, master_m, moment_q, moment_m, second_q, second_m,
    weight_q, weight_m, shard_q, shard_m, first_q, first_m, variance_q, variance_m,
    raw_m, turned_m, raw_q, relay, raw_in, sum_in, sum_out, partial, send_s, t_buf, u_buf, v_buf, state, gather_m,
    plane_buf, column_buf, row_buf,
    load_sem, rs_send, rs_recv, second_send, second_recv, ag_send, ag_recv, ar_send, ar_recv, hand,
):
    x, y = lax.axis_index("x"), lax.axis_index("y")
    z, c = lax.axis_index("z"), lax.axis_index("c")
    first_axis, second_axis = ("y", "x"), ("x", "y")
    f, s = (y, x), (x, y)

    def shard_index(a, fi, si):
        return si * N + fi if a == 0 else fi * N + si

    plane_peers, column_peers = [], []
    me_plane, me_column = x * N + y, z * 2 + c
    for d in range(1, 16):
        peer = lax.rem(me_plane + d, 16)
        plane_peers.append({"x": peer // N, "y": lax.rem(peer, N), "z": z, "c": c})
        peer = lax.rem(me_column + d, 16)
        column_peers.append({"x": x, "y": y, "z": peer // 2, "c": lax.rem(peer, 2)})

    def group_cols(fi):
        return pl.ds(pl.multiple_of(fi * GROUP, 128), GROUP)

    raw_loads = []
    for d in (2, 1, 3, 0):
        fi = wrap(x + d)
        copy = pltpu.make_async_copy(
            grads_m.at[:, group_cols(fi)], raw_m.at[:, group_cols(fi)], load_sem.at[d]
        )
        copy.start()
        raw_loads.append(copy)

    barrier = pltpu.get_barrier_semaphore()
    near_z = ({"z": lax.rem(z + 1, 8)}, {"z": lax.rem(z + 7, 8)})
    for peer in (
        {"x": wrap(x + 1)}, {"x": wrap(x + 3)}, {"y": wrap(y + 1)}, {"y": wrap(y + 3)}, *near_z
    ):
        pl.semaphore_signal(barrier, inc=1, device_id=peer, device_id_type=MESH_ID)

    @pl.when(c == 0)
    def _():
        pl.semaphore_signal(barrier, inc=1, device_id={"c": 1}, device_id_type=MESH_ID)

    query_loads = []
    for k in range(N):
        rows = pl.ds(pl.multiple_of(wrap(x + OFFSETS[k]) * GROUP, GROUP), GROUP)
        copy = pltpu.make_async_copy(grads_q.at[rows], raw_q.at[rows], load_sem.at[4 + k])
        copy.start()
        query_loads.append(copy)
    state_loads = []
    for i, ref in enumerate(
        (accum_q, accum_m, master_q, master_m, moment_q, moment_m, second_q, second_m)
    ):
        copy = pltpu.make_async_copy(ref, state.at[i], load_sem.at[8 + i])
        copy.start()
        state_loads.append(copy)

    pl.semaphore_wait(barrier, 6 + c)

    def near_signal(r):
        for peer in near_z:
            pl.semaphore_signal(hand.at[r], inc=1, device_id=peer, device_id_type=MESH_ID)

    def near_wait(r):
        pl.semaphore_wait(hand.at[r], 2)

    def partner_signal():
        pl.semaphore_signal(hand.at[3], inc=1, device_id={"c": 1 - c}, device_id_type=MESH_ID)

    def remote(src, dst, send, recv, axis, coordinate):
        return pltpu.make_async_remote_copy(
            src_ref=src,
            dst_ref=dst,
            send_sem=send,
            recv_sem=recv,
            device_id={axis: coordinate},
            device_id_type=MESH_ID,
        )

    started = []

    def go(copy):
        copy.start()
        started.append(copy)

    source = (raw_q, turned_m)
    low, high = pl.ds(0, HALF), pl.ds(HALF, HALF)

    def place(a, k):
        fi, si = f[a], wrap(s[a] + OFFSETS[k])
        return wrap(fi + 1), wrap(fi + 3), wrap(fi + 2), si

    def rs_copy(a, k, kind):
        plus, minus, far, si = place(a, k)

        def mine(owner, start):
            return source[a].at[shard_rows(shard_index(a, owner, si), start, HALF)]

        src, dst = {
            RELAY_A: lambda: (mine(far, 0), relay.at[a, k, 0]),
            RELAY_B: lambda: (mine(far, HALF), relay.at[a, k, 1]),
            RAW_P: lambda: (mine(plus, HALF), raw_in.at[a, k, 0]),
            RAW_M: lambda: (mine(minus, 0), raw_in.at[a, k, 1]),
            SUM_P: lambda: (sum_out.at[a, k, 0], sum_in.at[a, k, 0]),
            SUM_M: lambda: (sum_out.at[a, k, 1], sum_in.at[a, k, 1]),
        }[kind]()
        target = plus if kind in (RELAY_A, RAW_P, SUM_P) else minus
        return remote(
            src, dst, rs_send.at[a, k, kind], rs_recv.at[a, k, kind], first_axis[a], target
        )

    def raw_relay(a, k):
        if a == 0:
            query_loads[k].wait()
        go(rs_copy(a, k, RELAY_A))
        go(rs_copy(a, k, RELAY_B))

    def raw_direct(a, k):
        go(rs_copy(a, k, RAW_P))
        go(rs_copy(a, k, RAW_M))

    def as_f32(value):
        return value.astype(jnp.float32)

    def pass_on(a, k):
        plus, minus, far, si = place(a, k)
        for side, kind, owner, start in ((0, SUM_P, plus, 0), (1, SUM_M, minus, HALF)):
            rs_copy(a, k, RELAY_A + side).wait_recv()
            base = shard_index(a, owner, si) * ROWS + start

            def step(i, carry):
                at = pl.ds(pl.multiple_of(i * 16, 16), 16)
                mine = source[a][pl.ds(pl.multiple_of(base + i * 16, 16), 16), :]
                value = as_f32(mine) + as_f32(relay[a, k, side, at, :])
                sum_out[a, k, side, at, :] = value.astype(jnp.bfloat16)
                return carry

            lax.fori_loop(0, HALF // 16, step, 0)
            go(rs_copy(a, k, kind))

    def turn(fi):
        def step(i, carry):
            at = pl.ds(pl.multiple_of(fi * GROUP + i * 128, 128), 128)
            turned_m[at, :] = raw_m[:, at].T
            return carry

        lax.fori_loop(0, GROUP // 128, step, 0)

    def add_up(a, k):
        for kind in (RAW_P, RAW_M, SUM_P, SUM_M):
            rs_copy(a, k, kind).wait_recv()
        if k == 3:
            state_loads[a].wait()
        base = shard_index(a, f[a], wrap(s[a] + OFFSETS[k])) * ROWS
        for h in (0, 1):
            one = (sum_in, raw_in)[h]
            two = (raw_in, sum_in)[h]

            def step(i, carry):
                at = pl.ds(pl.multiple_of(i * 16, 16), 16)
                here = pl.ds(pl.multiple_of(h * HALF + i * 16, 16), 16)
                mine = source[a][pl.ds(pl.multiple_of(base + h * HALF + i * 16, 16), 16), :]
                value = as_f32(mine) + as_f32(one[a, k, 0, at, :]) + as_f32(two[a, k, 1, at, :])
                if k == 3:
                    partial[a, 1, here, :] = value + state[a, here, :]
                elif k == 0:
                    send_s[a, h, at, :] = value.astype(jnp.bfloat16)
                elif k == 1:
                    if h == 0:
                        partial[a, 0, here, :] = value
                    else:
                        send_s[a, 2, at, :] = value.astype(jnp.bfloat16)
                else:
                    if h == 0:
                        send_s[a, 3, at, :] = value.astype(jnp.bfloat16)
                    else:
                        partial[a, 0, here, :] = value
                return carry

            lax.fori_loop(0, HALF // 16, step, 0)

    def second_copy(a, kind):
        plus, minus = wrap(s[a] + 1), wrap(s[a] + 3)
        dst = (t_buf, u_buf, v_buf)[kind // 2].at[a, kind % 2]
        target = (plus, minus)[kind % 2]
        return remote(
            send_s.at[a, kind], dst,
            second_send.at[a, kind], second_recv.at[a, kind], second_axis[a], target,
        )

    def merge_t(a):
        for side, kind in ((0, V_P), (1, V_M)):
            second_copy(a, T_A + side).wait_recv()

            def step(i, carry):
                at = pl.ds(pl.multiple_of(i * 16, 16), 16)
                here = pl.ds(pl.multiple_of(side * HALF + i * 16, 16), 16)
                value = partial[a, 0, here, :] + as_f32(t_buf[a, side, at, :])
                send_s[a, kind, at, :] = value.astype(jnp.bfloat16)
                return carry

            lax.fori_loop(0, HALF // 16, step, 0)
            go(second_copy(a, kind))

    def squares(value):
        return jnp.sum((value * value).reshape(-1, 8, COLS), axis=0)

    def finish(a, acc):
        for kind in (U_P, U_M, V_P, V_M):
            second_copy(a, kind).wait_recv()
        for h, one, two in ((0, v_buf, u_buf), (1, u_buf, v_buf)):
            def step(i, acc):
                at = pl.ds(pl.multiple_of(i * 16, 16), 16)
                here = pl.ds(pl.multiple_of(h * HALF + i * 16, 16), 16)
                total = partial[a, 1, here, :] + as_f32(one[a, 0, at, :]) + as_f32(two[a, 1, at, :])
                partial[a, 1, here, :] = total
                return acc + squares(total)

            acc = lax.fori_loop(0, HALF // 16, step, acc)
        return acc

    for k in (0, 1):
        raw_relay(0, k)
        raw_direct(0, k)
    raw_loads[0].wait()
    turn(wrap(x + 2))
    raw_relay(1, 0)
    raw_relay(1, 1)
    near_signal(0)
    raw_loads[1].wait()
    turn(wrap(x + 1))
    raw_loads[2].wait()
    turn(wrap(x + 3))
    raw_direct(1, 0)
    raw_direct(1, 1)
    for a in (0, 1):
        pass_on(a, 0)
        raw_relay(a, 2)
        raw_direct(a, 2)
    near_wait(0)
    near_signal(1)
    raw_loads[3].wait()
    turn(x)
    for a in (0, 1):
        pass_on(a, 1)
        raw_relay(a, 3)
        raw_direct(a, 3)
    near_wait(1)
    near_signal(2)
    for a in (0, 1):
        pass_on(a, 2)
        add_up(a, 0)
        go(second_copy(a, T_A))
        go(second_copy(a, T_B))
    near_wait(2)

    @pl.when(c == 1)
    def _():
        partner_signal()

    for a in (0, 1):
        pass_on(a, 3)
        add_up(a, 1)
        go(second_copy(a, U_P))
    for a in (0, 1):
        add_up(a, 2)
        go(second_copy(a, U_M))
    for a in (0, 1):
        merge_t(a)
    for a in (0, 1):
        add_up(a, 3)

    @pl.when(c == 0)
    def _():
        pl.semaphore_wait(hand.at[3], 1)
        partner_signal()

    acc = jnp.zeros((8, COLS), jnp.float32)
    for a in (0, 1):
        acc = finish(a, acc)

    @pl.when(c == 1)
    def _():
        pl.semaphore_wait(hand.at[3], 1)

    def exchange(stage, row, buf, me, peers):
        row_buf[stage] = row
        buf[me] = row
        for d, peer in enumerate(peers):
            copy = pltpu.make_async_remote_copy(
                src_ref=row_buf.at[stage],
                dst_ref=buf.at[me],
                send_sem=ar_send.at[stage, d],
                recv_sem=ar_recv.at[stage, d],
                device_id=peer,
                device_id_type=MESH_ID,
            )
            go(copy)
        for d in range(15):
            sender = lax.rem(me + 15 - d, 16)
            pltpu.make_async_remote_copy(
                src_ref=row_buf.at[stage],
                dst_ref=buf.at[sender],
                send_sem=ar_send.at[stage, d],
                recv_sem=ar_recv.at[stage, d],
                device_id=peers[d],
                device_id_type=MESH_ID,
            ).wait_recv()
        return jnp.sum(buf[...], axis=0)

    row = jnp.sum(acc, axis=0, keepdims=True)
    row = row[:, :128] + row[:, 128:]
    row = exchange(0, row, plane_buf, me_plane, plane_peers)
    row = exchange(1, row, column_buf, me_column, column_peers)
    sumsq = jnp.sum(row, axis=1, keepdims=True)
    clip = jnp.minimum(1.0, lax.rsqrt(sumsq / float(ENTRIES) + 1e-06))

    gathered = (weight_q, gather_m)
    outs = ((shard_q, first_q, variance_q), (shard_m, first_m, variance_m))
    for copy in state_loads[2:]:
        copy.wait()

    def update(a):
        base = shard_index(a, f[a], s[a]) * ROWS
        shard_out, first_out, variance_out = outs[a]

        def step(i, carry):
            at = pl.ds(pl.multiple_of(i * BLOCK, BLOCK), BLOCK)
            scaled = clip * partial[a, 1, at, :]
            master = state[2 + a, at, :]
            first = BETA_ONE * state[4 + a, at, :] + (1.0 - BETA_ONE) * scaled
            variance = BETA_TWO * state[6 + a, at, :] + (1.0 - BETA_TWO) * scaled * scaled
            corr_one = 1.0 - BETA_ONE**STEP
            corr_two = 1.0 - BETA_TWO**STEP
            change = (
                first / corr_one / (jnp.sqrt(variance / corr_two) + ADAM_EPS)
                + WEIGHT_DECAY * master
            )
            shard = master - LEARN_RATE * change
            shard_out[at, :] = shard
            first_out[at, :] = first
            variance_out[at, :] = variance
            gathered[a][pl.ds(pl.multiple_of(base + i * BLOCK, BLOCK), BLOCK), :] = shard.astype(
                jnp.bfloat16
            )
            return carry

        lax.fori_loop(0, ROWS // BLOCK, step, 0)

    ITEMS = (0, 3, 1, 2)

    def ag_copy(a, item, kind):
        if item == 0:
            axis, here = second_axis[a], s[a]
        else:
            axis, here = first_axis[a], f[a]
        owner = {0: here, 1: here, 2: wrap(here + 3), 3: wrap(here + 1)}[kind]
        if item == 0:
            index = shard_index(a, f[a], owner)
        else:
            index = shard_index(a, owner, wrap(s[a] + ITEMS[item - 1]))
        start, size = {0: (0, ROWS), 1: (0, ROWS), 2: (0, HALF), 3: (HALF, HALF)}[kind]
        ref = gathered[a].at[shard_rows(index, start, size)]
        target = wrap(here + 1) if kind in (0, 2) else wrap(here + 3)
        return remote(ref, ref, ag_send.at[a, item, kind], ag_recv.at[a, item, kind], axis, target)

    def ag_wait(a, item, kind):
        if item == 0:
            axis, here = second_axis[a], s[a]
        else:
            axis, here = first_axis[a], f[a]
        owner = {0: wrap(here + 3), 1: wrap(here + 1), 2: wrap(here + 2), 3: wrap(here + 2)}[kind]
        if item == 0:
            index = shard_index(a, f[a], owner)
        else:
            index = shard_index(a, owner, wrap(s[a] + ITEMS[item - 1]))
        start, size = {0: (0, ROWS), 1: (0, ROWS), 2: (0, HALF), 3: (HALF, HALF)}[kind]
        ref = gathered[a].at[shard_rows(index, start, size)]
        remote(
            ref, ref, ag_send.at[a, item, kind], ag_recv.at[a, item, kind], axis, here
        ).wait_recv()

    def turn_back(fi):
        def step(i, carry):
            at = pl.ds(pl.multiple_of(fi * GROUP + i * 128, 128), 128)
            weight_m[:, at] = gather_m[at, :].T
            return carry

        lax.fori_loop(0, GROUP // 128, step, 0)

    for a in (0, 1):
        update(a)
        for item in (0, 1):
            go(ag_copy(a, item, 0))
            go(ag_copy(a, item, 1))
    for a in (0, 1):
        ag_wait(a, 0, 0)
        go(ag_copy(a, 0, 2))
        ag_wait(a, 0, 1)
        go(ag_copy(a, 0, 3))
        for item in (2, 3):
            go(ag_copy(a, item, 0))
            go(ag_copy(a, item, 1))

    def ag_forward(a, item):
        ag_wait(a, item, 0)
        go(ag_copy(a, item, 2))
        ag_wait(a, item, 1)
        go(ag_copy(a, item, 3))

    for a in (0, 1):
        ag_forward(a, 1)
    for a in (0, 1):
        ag_wait(a, 0, 2)
        ag_wait(a, 0, 3)
        go(ag_copy(a, 4, 0))
        go(ag_copy(a, 4, 1))
    turn_back(x)
    for item in (2, 3, 4):
        for a in (0, 1):
            ag_forward(a, item)
    turn_back(wrap(x + 1))
    turn_back(wrap(x + 3))
    for item in (1, 2, 3, 4):
        for a in (0, 1):
            ag_wait(a, item, 2)
            ag_wait(a, item, 3)
    turn_back(wrap(x + 2))
    for copy in started:
        copy.wait_send()


def write_out(*refs):
    sources, targets, sem = refs[:8], refs[8:16], refs[16]
    copies = [
        pltpu.make_async_copy(source, target, sem.at[i])
        for i, (source, target) in enumerate(zip(sources, targets))
    ]
    for copy in copies:
        copy.start()
    for copy in copies:
        copy.wait()


def on_device(
    query_grads, merge_grads, query_accum, merge_accum, query_master, merge_master,
    query_moment, merge_moment, query_second, merge_second,
):
    def flat(value):
        return value.reshape(ROWS, COLS)

    def turned(value):
        return jnp.swapaxes(value[0], 0, 1)

    bf16, f32 = jnp.bfloat16, jnp.float32
    hbm_spec = pl.BlockSpec(memory_space=pltpu.HBM)
    shard = pltpu.VMEM((ROWS, COLS), f32)
    operands = (
        query_grads.reshape(FULL, COLS), merge_grads.reshape(COLS, FULL),
        flat(query_accum), turned(merge_accum), flat(query_master), turned(merge_master),
        flat(query_moment), turned(merge_moment), flat(query_second), turned(merge_second),
    )
    operands = [pltpu.with_memory_space_constraint(value, pltpu.HBM) for value in operands]
    outs = pl.pallas_call(
        kernel,
        name="adamw_step",
        out_shape=[
            pltpu.VMEM((FULL, COLS), bf16),
            pltpu.VMEM((COLS, FULL), bf16),
            shard, shard, shard, shard, shard, shard,
        ],
        in_specs=[hbm_spec] * 10,
        out_specs=[pl.BlockSpec(memory_space=pltpu.VMEM)] * 8,
        scratch_shapes=[
            pltpu.VMEM((COLS, FULL), bf16),
            pltpu.VMEM((FULL, COLS), bf16),
            pltpu.VMEM((FULL, COLS), bf16),
            pltpu.VMEM((2, N, 2, HALF, COLS), bf16),
            pltpu.VMEM((2, N, 2, HALF, COLS), bf16),
            pltpu.VMEM((2, N, 2, HALF, COLS), bf16),
            pltpu.VMEM((2, N, 2, HALF, COLS), bf16),
            pltpu.VMEM((2, 2, ROWS, COLS), f32),
            pltpu.VMEM((2, 6, HALF, COLS), bf16),
            pltpu.VMEM((2, 2, HALF, COLS), bf16),
            pltpu.VMEM((2, 2, HALF, COLS), bf16),
            pltpu.VMEM((2, 2, HALF, COLS), bf16),
            pltpu.VMEM((8, ROWS, COLS), f32),
            pltpu.VMEM((FULL, COLS), bf16),
            pltpu.VMEM((16, 1, 128), f32),
            pltpu.VMEM((16, 1, 128), f32),
            pltpu.VMEM((2, 1, 128), f32),
            pltpu.SemaphoreType.DMA((16,)),
            pltpu.SemaphoreType.DMA((2, N, 6)),
            pltpu.SemaphoreType.DMA((2, N, 6)),
            pltpu.SemaphoreType.DMA((2, 6)),
            pltpu.SemaphoreType.DMA((2, 6)),
            pltpu.SemaphoreType.DMA((2, 5, 4)),
            pltpu.SemaphoreType.DMA((2, 5, 4)),
            pltpu.SemaphoreType.DMA((2, 15)),
            pltpu.SemaphoreType.DMA((2, 15)),
            pltpu.SemaphoreType.REGULAR((4,)),
        ],
        compiler_params=pltpu.CompilerParams(
            collective_id=0, has_side_effects=True, vmem_limit_bytes=32 * 2**20
        ),
    )(*operands)
    outs = pl.pallas_call(
        write_out,
        name="write_out",
        out_shape=[jax.ShapeDtypeStruct(out.shape, out.dtype) for out in outs],
        in_specs=[pl.BlockSpec(memory_space=pltpu.VMEM)] * 8,
        out_specs=[hbm_spec] * 8,
        scratch_shapes=[pltpu.SemaphoreType.DMA((8,))],
        compiler_params=pltpu.CompilerParams(vmem_limit_bytes=2**20),
    )(*outs)
    weight_q, weight_m, shard_q, shard_m, first_q, first_m, variance_q, variance_m = outs

    def back(value):
        return jnp.swapaxes(value, 0, 1)[None]

    return (
        weight_q[None], weight_m[None],
        shard_q[None], back(shard_m), first_q[None], back(first_m), variance_q[None], back(variance_m),
    )


def solution(mesh):
    finer = Mesh(mesh.devices.reshape(4, 4, 8, 2), ("x", "y", "z", "c"))
    dp, mp = ("x", "y"), ("z", "c")
    query, merge = P(None, dp, mp), P(None, mp, dp)
    return jax.shard_map(
        on_device,
        mesh=finer,
        in_specs=(P(dp, None, None, mp), P(dp, None, mp, None)) + (query, merge) * 4,
        out_specs=(P(None, None, mp), P(None, mp, None)) + (query, merge) * 3,
        check_vma=False,
    )
```

```python
import jax
import jax.numpy as jnp
from jax import lax
from jax.experimental import pallas as pl
from jax.experimental.pallas import tpu as pltpu
from jax.sharding import Mesh
from jax.sharding import PartitionSpec as P

STEP = 10
ENTRIES = 29360128
BETA_ONE = 0.9
BETA_TWO = 0.95
LEARN_RATE = 0.002
WEIGHT_DECAY = 0.1
ADAM_EPS = 1e-08

N = 4
ROWS = 224
COLS = 256
HALF = ROWS // 2
GROUP = N * ROWS
FULL = N * GROUP
BLOCK = 32
MESH_ID = pl.DeviceIdType.MESH
OFFSETS = (2, 1, 3, 0)

RELAY_A, RELAY_B, RAW_P, RAW_M, SUM_P, SUM_M = range(6)
T_A, T_B, U_P, U_M, V_P, V_M = range(6)


def wrap(value):
    return lax.rem(value, N)


def each_block(count, step, carry):
    for i in range(count):
        carry = step(i, carry)
    return carry


def shard_rows(index, start=0, size=ROWS):
    return pl.ds(pl.multiple_of(index * ROWS + start, 16), size)


def kernel(
    grads_q, grads_m, accum_q, accum_m, master_q, master_m, moment_q, moment_m, second_q, second_m,
    weight_q, weight_m, shard_q, shard_m, first_q, first_m, variance_q, variance_m,
    raw_m, turned_m, raw_q, relay, raw_in, sum_in, sum_out, partial, send_s, t_buf, u_buf, v_buf, state, gather_m,
    plane_buf, column_buf, row_buf,
    load_sem, rs_send, rs_recv, second_recv, ag_send, ag_recv, ar_send, ar_recv, hand,
):
    x, y = lax.axis_index("x"), lax.axis_index("y")
    z, c = lax.axis_index("z"), lax.axis_index("c")
    first_axis, second_axis = ("y", "x"), ("x", "y")
    f, s = (y, x), (x, y)

    def shard_index(a, fi, si):
        return si * N + fi if a == 0 else fi * N + si

    plane_peers, column_peers = [], []
    me_plane, me_column = x * N + y, z * 2 + c
    for d in range(1, 16):
        peer = lax.rem(me_plane + d, 16)
        plane_peers.append({"x": peer // N, "y": lax.rem(peer, N), "z": z, "c": c})
        peer = lax.rem(me_column + d, 16)
        column_peers.append({"x": x, "y": y, "z": peer // 2, "c": lax.rem(peer, 2)})

    def group_cols(fi):
        return pl.ds(pl.multiple_of(fi * GROUP, 128), GROUP)

    raw_loads = []
    for d in (2, 1, 3, 0):
        fi = wrap(x + d)
        copy = pltpu.make_async_copy(
            grads_m.at[:, group_cols(fi)], raw_m.at[:, group_cols(fi)], load_sem.at[d]
        )
        copy.start()
        raw_loads.append(copy)

    barrier = pltpu.get_barrier_semaphore()
    near_z = ({"z": lax.rem(z + 1, 8)}, {"z": lax.rem(z + 7, 8)})
    for peer in (
        {"x": wrap(x + 1)}, {"x": wrap(x + 3)}, {"y": wrap(y + 1)}, {"y": wrap(y + 3)}, *near_z
    ):
        pl.semaphore_signal(barrier, inc=1, device_id=peer, device_id_type=MESH_ID)

    @pl.when(c == 0)
    def _():
        pl.semaphore_signal(barrier, inc=1, device_id={"c": 1}, device_id_type=MESH_ID)

    query_loads = []
    for k in range(N):
        rows = pl.ds(pl.multiple_of(wrap(x + OFFSETS[k]) * GROUP, GROUP), GROUP)
        copy = pltpu.make_async_copy(grads_q.at[rows], raw_q.at[rows], load_sem.at[4 + k])
        copy.start()
        query_loads.append(copy)
    state_loads = []
    for i, ref in enumerate(
        (accum_q, accum_m, master_q, master_m, moment_q, moment_m, second_q, second_m)
    ):
        copy = pltpu.make_async_copy(ref, state.at[i], load_sem.at[8 + min(i, 2)])
        copy.start()
        state_loads.append(copy)

    pl.semaphore_wait(barrier, 6 + c)

    def near_signal(r):
        for peer in near_z:
            pl.semaphore_signal(hand.at[r], inc=1, device_id=peer, device_id_type=MESH_ID)

    def near_wait(r):
        pl.semaphore_wait(hand.at[r], 2)

    def partner_signal():
        pl.semaphore_signal(hand.at[3], inc=1, device_id={"c": 1 - c}, device_id_type=MESH_ID)

    def remote(src, dst, send, recv, axis, coordinate):
        return pltpu.make_async_remote_copy(
            src_ref=src,
            dst_ref=dst,
            send_sem=send,
            recv_sem=recv,
            device_id={axis: coordinate},
            device_id_type=MESH_ID,
        )

    def go(copy):
        copy.start()

    source = (raw_q, turned_m)
    low, high = pl.ds(0, HALF), pl.ds(HALF, HALF)

    def place(a, k):
        fi, si = f[a], wrap(s[a] + OFFSETS[k])
        return wrap(fi + 1), wrap(fi + 3), wrap(fi + 2), si

    def rs_copy(a, k, kind):
        plus, minus, far, si = place(a, k)

        def mine(owner, start):
            return source[a].at[shard_rows(shard_index(a, owner, si), start, HALF)]

        src, dst = {
            RELAY_A: lambda: (mine(far, 0), relay.at[a, k, 0]),
            RELAY_B: lambda: (mine(far, HALF), relay.at[a, k, 1]),
            RAW_P: lambda: (mine(plus, HALF), raw_in.at[a, k, 0]),
            RAW_M: lambda: (mine(minus, 0), raw_in.at[a, k, 1]),
            SUM_P: lambda: (sum_out.at[a, k, 0], sum_in.at[a, k, 0]),
            SUM_M: lambda: (sum_out.at[a, k, 1], sum_in.at[a, k, 1]),
        }[kind]()
        target = plus if kind in (RELAY_A, RAW_P, SUM_P) else minus
        return remote(
            src, dst, rs_send.at[a], rs_recv.at[a, k, min(kind, 2)], first_axis[a], target
        )

    def wait_bytes(ref, sem):
        pltpu.make_async_copy(ref, ref, sem).wait()

    def raw_relay(a, k):
        if a == 0:
            query_loads[k].wait()
        go(rs_copy(a, k, RELAY_A))
        go(rs_copy(a, k, RELAY_B))

    def raw_direct(a, k):
        go(rs_copy(a, k, RAW_P))
        go(rs_copy(a, k, RAW_M))

    def as_f32(value):
        return value.astype(jnp.float32)

    def pass_on(a, k):
        plus, minus, far, si = place(a, k)
        for side, kind, owner, start in ((0, SUM_P, plus, 0), (1, SUM_M, minus, HALF)):
            rs_copy(a, k, RELAY_A + side).wait_recv()
            base = shard_index(a, owner, si) * ROWS + start

            def step(i, carry):
                at = pl.ds(i * 16, 16)
                mine = source[a][pl.ds(pl.multiple_of(base + i * 16, 16), 16), :]
                value = as_f32(mine) + as_f32(relay[a, k, side, at, :])
                sum_out[a, k, side, at, :] = value.astype(jnp.bfloat16)
                return carry

            each_block(HALF // 16, step, 0)
            go(rs_copy(a, k, kind))

    def turn(fi):
        def step(i, carry):
            at = pl.ds(pl.multiple_of(fi * GROUP + i * 128, 128), 128)
            turned_m[at, :] = raw_m[:, at].T
            return carry

        lax.fori_loop(0, GROUP // 128, step, 0)

    def add_up(a, k):
        wait_bytes(source[a].at[pl.ds(0, 2 * ROWS)], rs_recv.at[a, k, 2])
        if k == 3:
            state_loads[a].wait()
        base = shard_index(a, f[a], wrap(s[a] + OFFSETS[k])) * ROWS
        for h in (0, 1):
            one = (sum_in, raw_in)[h]
            two = (raw_in, sum_in)[h]

            def step(i, carry):
                at = pl.ds(i * 16, 16)
                here = pl.ds(h * HALF + i * 16, 16)
                mine = source[a][pl.ds(pl.multiple_of(base + h * HALF + i * 16, 16), 16), :]
                value = as_f32(mine) + as_f32(one[a, k, 0, at, :]) + as_f32(two[a, k, 1, at, :])
                if k == 3:
                    partial[a, 1, here, :] = value + state[a, here, :]
                elif k == 0:
                    send_s[a, h, at, :] = value.astype(jnp.bfloat16)
                elif k == 1:
                    if h == 0:
                        partial[a, 0, here, :] = value
                    else:
                        send_s[a, 2, at, :] = value.astype(jnp.bfloat16)
                else:
                    if h == 0:
                        send_s[a, 3, at, :] = value.astype(jnp.bfloat16)
                    else:
                        partial[a, 0, here, :] = value
                return carry

            each_block(HALF // 16, step, 0)

    def second_copy(a, kind):
        plus, minus = wrap(s[a] + 1), wrap(s[a] + 3)
        dst = (t_buf, u_buf, v_buf)[kind // 2].at[a, kind % 2]
        target = (plus, minus)[kind % 2]
        return remote(
            send_s.at[a, kind], dst,
            rs_send.at[a], second_recv.at[a, min(kind, 2)], second_axis[a], target,
        )

    def merge_t(a):
        for side, kind in ((0, V_P), (1, V_M)):
            second_copy(a, T_A + side).wait_recv()

            def step(i, carry):
                at = pl.ds(i * 16, 16)
                here = pl.ds(side * HALF + i * 16, 16)
                value = partial[a, 0, here, :] + as_f32(t_buf[a, side, at, :])
                send_s[a, kind, at, :] = value.astype(jnp.bfloat16)
                return carry

            each_block(HALF // 16, step, 0)
            go(second_copy(a, kind))

    def squares(value):
        return jnp.sum((value * value).reshape(-1, 8, COLS), axis=0)

    def finish(a, acc):
        wait_bytes(source[a].at[pl.ds(0, 2 * ROWS)], second_recv.at[a, 2])
        for h, one, two in ((0, v_buf, u_buf), (1, u_buf, v_buf)):
            def step(i, acc):
                at = pl.ds(i * 16, 16)
                here = pl.ds(h * HALF + i * 16, 16)
                total = partial[a, 1, here, :] + as_f32(one[a, 0, at, :]) + as_f32(two[a, 1, at, :])
                partial[a, 1, here, :] = total
                return acc + squares(total)

            acc = each_block(HALF // 16, step, acc)
        return acc

    raw_relay(0, 0)
    raw_relay(0, 1)
    raw_direct(0, 0)
    raw_relay(0, 2)
    raw_loads[0].wait()
    turn(wrap(x + 2))
    raw_relay(1, 0)
    raw_relay(1, 1)
    near_signal(0)
    raw_loads[1].wait()
    turn(wrap(x + 1))
    raw_loads[2].wait()
    turn(wrap(x + 3))
    raw_direct(1, 0)
    raw_relay(1, 2)
    for k in (0, 1):
        for a in (0, 1):
            pass_on(a, k)
            raw_direct(a, k + 1)
    near_wait(0)
    near_signal(1)
    raw_loads[3].wait()
    turn(x)
    for a in (0, 1):
        pass_on(a, 2)
    for a in (0, 1):
        add_up(a, 0)
        go(second_copy(a, T_A))
        go(second_copy(a, T_B))
    near_wait(1)
    near_signal(2)
    for a in (0, 1):
        add_up(a, 1)
        go(second_copy(a, U_P))
        raw_relay(a, 3)
        raw_direct(a, 3)
    for a in (0, 1):
        add_up(a, 2)
        go(second_copy(a, U_M))
    for a in (0, 1):
        merge_t(a)
    near_wait(2)

    @pl.when(c == 1)
    def _():
        partner_signal()

    for a in (0, 1):
        pass_on(a, 3)

    @pl.when(c == 0)
    def _():
        pl.semaphore_wait(hand.at[3], 1)
        partner_signal()

    for a in (0, 1):
        add_up(a, 3)

    acc = jnp.zeros((8, COLS), jnp.float32)
    for a in (0, 1):
        acc = finish(a, acc)

    @pl.when(c == 1)
    def _():
        pl.semaphore_wait(hand.at[3], 1)

    def exchange(stage, row, buf, me, peers):
        row_buf[stage] = row
        buf[me] = row
        for peer in peers:
            go(
                pltpu.make_async_remote_copy(
                    src_ref=row_buf.at[stage],
                    dst_ref=buf.at[me],
                    send_sem=ar_send.at[stage],
                    recv_sem=ar_recv.at[stage],
                    device_id=peer,
                    device_id_type=MESH_ID,
                )
            )
        wait_bytes(buf.at[pl.ds(0, 15)], ar_recv.at[stage])
        return jnp.sum(buf[...], axis=0)

    row = jnp.sum(acc, axis=0, keepdims=True)
    row = row[:, :128] + row[:, 128:]
    row = exchange(0, row, plane_buf, me_plane, plane_peers)
    row = exchange(1, row, column_buf, me_column, column_peers)
    sumsq = jnp.sum(row, axis=1, keepdims=True)
    clip = jnp.minimum(1.0, lax.rsqrt(sumsq / float(ENTRIES) + 1e-06))

    gathered = (weight_q, gather_m)
    outs = ((shard_q, first_q, variance_q), (shard_m, first_m, variance_m))
    pltpu.make_async_copy(state.at[pl.ds(2, 6)], state.at[pl.ds(2, 6)], load_sem.at[10]).wait()

    def update(a):
        base = shard_index(a, f[a], s[a]) * ROWS
        shard_out, first_out, variance_out = outs[a]

        def step(i, carry):
            at = pl.ds(i * BLOCK, BLOCK)
            scaled = clip * partial[a, 1, at, :]
            master = state[2 + a, at, :]
            first = BETA_ONE * state[4 + a, at, :] + (1.0 - BETA_ONE) * scaled
            variance = BETA_TWO * state[6 + a, at, :] + (1.0 - BETA_TWO) * scaled * scaled
            corr_one = 1.0 - BETA_ONE**STEP
            corr_two = 1.0 - BETA_TWO**STEP
            change = (
                first / corr_one / (jnp.sqrt(variance / corr_two) + ADAM_EPS)
                + WEIGHT_DECAY * master
            )
            shard = master - LEARN_RATE * change
            shard_out[at, :] = shard
            first_out[at, :] = first
            variance_out[at, :] = variance
            gathered[a][pl.ds(pl.multiple_of(base + i * BLOCK, BLOCK), BLOCK), :] = shard.astype(
                jnp.bfloat16
            )
            return carry

        each_block(ROWS // BLOCK, step, 0)

    ITEMS = (0, 3, 1, 2)

    def ag_copy(a, item, kind):
        if item == 0:
            axis, here = second_axis[a], s[a]
        else:
            axis, here = first_axis[a], f[a]
        owner = {0: here, 1: here, 2: wrap(here + 3), 3: wrap(here + 1)}[kind]
        if item == 0:
            index = shard_index(a, f[a], owner)
        else:
            index = shard_index(a, owner, wrap(s[a] + ITEMS[item - 1]))
        start, size = {0: (0, ROWS), 1: (0, ROWS), 2: (0, HALF), 3: (HALF, HALF)}[kind]
        ref = gathered[a].at[shard_rows(index, start, size)]
        target = wrap(here + 1) if kind in (0, 2) else wrap(here + 3)
        if kind < 2:
            slot = 2 * item + kind
        else:
            slot = 10 if item == 0 else 11
        return remote(ref, ref, ag_send.at[a], ag_recv.at[a, slot], axis, target)

    def ag_wait(a, item, kind):
        wait_bytes(gathered[a].at[pl.ds(0, ROWS)], ag_recv.at[a, 2 * item + kind])

    def ag_wait_far(a, along_first):
        count = N * ROWS if along_first else ROWS
        wait_bytes(gathered[a].at[pl.ds(0, count)], ag_recv.at[a, 11 if along_first else 10])

    def turn_back(fi):
        def step(i, carry):
            at = pl.ds(pl.multiple_of(fi * GROUP + i * 128, 128), 128)
            weight_m[:, at] = gather_m[at, :].T
            return carry

        lax.fori_loop(0, GROUP // 128, step, 0)

    for a in (0, 1):
        update(a)
        for item in (0, 1):
            go(ag_copy(a, item, 0))
            go(ag_copy(a, item, 1))
    def ag_forward(a, item):
        ag_wait(a, item, 0)
        go(ag_copy(a, item, 2))
        ag_wait(a, item, 1)
        go(ag_copy(a, item, 3))

    for a in (0, 1):
        ag_forward(a, 0)
    for item in (2, 3):
        for a in (0, 1):
            go(ag_copy(a, item, 0))
            go(ag_copy(a, item, 1))
    for a in (0, 1):
        ag_forward(a, 1)
    for a in (0, 1):
        ag_wait_far(a, False)
        go(ag_copy(a, 4, 0))
        go(ag_copy(a, 4, 1))
    turn_back(x)
    for item in (2, 3, 4):
        for a in (0, 1):
            ag_forward(a, item)
    turn_back(wrap(x + 1))
    turn_back(wrap(x + 3))
    ag_wait_far(1, True)
    turn_back(wrap(x + 2))
    ag_wait_far(0, True)
    for a in (0, 1):
        wait_bytes(gathered[a].at[pl.ds(0, 15 * ROWS)], ag_send.at[a])
        wait_bytes(gathered[a].at[pl.ds(0, 15 * ROWS)], rs_send.at[a])
        wait_bytes(plane_buf.at[pl.ds(0, 15)], ar_send.at[a])


def write_out(*refs):
    sources, targets, sem = refs[:8], refs[8:16], refs[16]
    copies = [
        pltpu.make_async_copy(source, target, sem.at[i])
        for i, (source, target) in enumerate(zip(sources, targets))
    ]
    for copy in copies:
        copy.start()
    for copy in copies:
        copy.wait()


def on_device(
    query_grads, merge_grads, query_accum, merge_accum, query_master, merge_master,
    query_moment, merge_moment, query_second, merge_second,
):
    def flat(value):
        return value.reshape(ROWS, COLS)

    def turned(value):
        return jnp.swapaxes(value[0], 0, 1)

    bf16, f32 = jnp.bfloat16, jnp.float32
    hbm_spec = pl.BlockSpec(memory_space=pltpu.HBM)
    shard = pltpu.VMEM((ROWS, COLS), f32)
    operands = (
        query_grads.reshape(FULL, COLS), merge_grads.reshape(COLS, FULL),
        flat(query_accum), turned(merge_accum), flat(query_master), turned(merge_master),
        flat(query_moment), turned(merge_moment), flat(query_second), turned(merge_second),
    )
    operands = [pltpu.with_memory_space_constraint(value, pltpu.HBM) for value in operands]
    outs = pl.pallas_call(
        kernel,
        name="adamw_step",
        out_shape=[
            pltpu.VMEM((FULL, COLS), bf16),
            pltpu.VMEM((COLS, FULL), bf16),
            shard, shard, shard, shard, shard, shard,
        ],
        in_specs=[hbm_spec] * 10,
        out_specs=[pl.BlockSpec(memory_space=pltpu.VMEM)] * 8,
        scratch_shapes=[
            pltpu.VMEM((COLS, FULL), bf16),
            pltpu.VMEM((FULL, COLS), bf16),
            pltpu.VMEM((FULL, COLS), bf16),
            pltpu.VMEM((2, N, 2, HALF, COLS), bf16),
            pltpu.VMEM((2, N, 2, HALF, COLS), bf16),
            pltpu.VMEM((2, N, 2, HALF, COLS), bf16),
            pltpu.VMEM((2, N, 2, HALF, COLS), bf16),
            pltpu.VMEM((2, 2, ROWS, COLS), f32),
            pltpu.VMEM((2, 6, HALF, COLS), bf16),
            pltpu.VMEM((2, 2, HALF, COLS), bf16),
            pltpu.VMEM((2, 2, HALF, COLS), bf16),
            pltpu.VMEM((2, 2, HALF, COLS), bf16),
            pltpu.VMEM((8, ROWS, COLS), f32),
            pltpu.VMEM((FULL, COLS), bf16),
            pltpu.VMEM((16, 1, 128), f32),
            pltpu.VMEM((16, 1, 128), f32),
            pltpu.VMEM((2, 1, 128), f32),
            pltpu.SemaphoreType.DMA((11,)),
            pltpu.SemaphoreType.DMA((2,)),
            pltpu.SemaphoreType.DMA((2, N, 3)),
            pltpu.SemaphoreType.DMA((2, 3)),
            pltpu.SemaphoreType.DMA((2,)),
            pltpu.SemaphoreType.DMA((2, 12)),
            pltpu.SemaphoreType.DMA((2,)),
            pltpu.SemaphoreType.DMA((2,)),
            pltpu.SemaphoreType.REGULAR((4,)),
        ],
        compiler_params=pltpu.CompilerParams(
            collective_id=0, has_side_effects=True, vmem_limit_bytes=32 * 2**20
        ),
    )(*operands)
    outs = pl.pallas_call(
        write_out,
        name="write_out",
        out_shape=[jax.ShapeDtypeStruct(out.shape, out.dtype) for out in outs],
        in_specs=[pl.BlockSpec(memory_space=pltpu.VMEM)] * 8,
        out_specs=[hbm_spec] * 8,
        scratch_shapes=[pltpu.SemaphoreType.DMA((8,))],
        compiler_params=pltpu.CompilerParams(vmem_limit_bytes=2**20),
    )(*outs)
    weight_q, weight_m, shard_q, shard_m, first_q, first_m, variance_q, variance_m = outs

    def back(value):
        return jnp.swapaxes(value, 0, 1)[None]

    return (
        weight_q[None], weight_m[None],
        shard_q[None], back(shard_m), first_q[None], back(first_m), variance_q[None], back(variance_m),
    )


def solution(mesh):
    finer = Mesh(mesh.devices.reshape(4, 4, 8, 2), ("x", "y", "z", "c"))
    dp, mp = ("x", "y"), ("z", "c")
    query, merge = P(None, dp, mp), P(None, mp, dp)
    return jax.shard_map(
        on_device,
        mesh=finer,
        in_specs=(P(dp, None, None, mp), P(dp, None, mp, None)) + (query, merge) * 4,
        out_specs=(P(None, None, mp), P(None, mp, None)) + (query, merge) * 3,
        check_vma=False,
    )
```

```python
import jax
import jax.numpy as jnp
from jax import lax
from jax.experimental import pallas as pl
from jax.experimental.pallas import tpu as pltpu
from jax.sharding import Mesh
from jax.sharding import PartitionSpec as P

STEP = 10
ENTRIES = 29360128
BETA_ONE = 0.9
BETA_TWO = 0.95
LEARN_RATE = 0.002
WEIGHT_DECAY = 0.1
ADAM_EPS = 1e-08

N = 4
ROWS = 224
COLS = 256
HALF = ROWS // 2
GROUP = N * ROWS
FULL = N * GROUP
BLOCK = 32
MESH_ID = pl.DeviceIdType.MESH
OFFSETS = (2, 1, 3, 0)

RELAY_A, RELAY_B, RAW_P, RAW_M, SUM_P, SUM_M = range(6)
T_A, T_B, U_P, U_M, V_P, V_M = range(6)


def wrap(value):
    return lax.rem(value, N)


def each_block(count, step, carry):
    for i in range(count):
        carry = step(i, carry)
    return carry


def shard_rows(index, start=0, size=ROWS):
    return pl.ds(pl.multiple_of(index * ROWS + start, 16), size)


def kernel(
    grads_q, grads_m, accum_q, accum_m, master_q, master_m, moment_q, moment_m, second_q, second_m,
    weight_q, weight_m, shard_q, shard_m, first_q, first_m, variance_q, variance_m,
    raw_m, turned_m, raw_q, relay, raw_in, sum_in, sum_out, partial, send_s, t_buf, u_buf, v_buf, state, gather_m,
    plane_buf, column_buf, row_buf,
    load_sem, rs_send, rs_recv, second_recv, ag_send, ag_recv, ar_send, ar_recv, hand,
):
    x, y = lax.axis_index("x"), lax.axis_index("y")
    z, c = lax.axis_index("z"), lax.axis_index("c")
    first_axis, second_axis = ("y", "x"), ("x", "y")
    f, s = (y, x), (x, y)

    def shard_index(a, fi, si):
        return si * N + fi if a == 0 else fi * N + si

    plane_peers, column_peers = [], []
    me_plane, me_column = x * N + y, z * 2 + c
    for d in range(1, 16):
        peer = lax.rem(me_plane + d, 16)
        plane_peers.append({"x": peer // N, "y": lax.rem(peer, N), "z": z, "c": c})
        peer = lax.rem(me_column + d, 16)
        column_peers.append({"x": x, "y": y, "z": peer // 2, "c": lax.rem(peer, 2)})

    def group_cols(fi):
        return pl.ds(pl.multiple_of(fi * GROUP, 128), GROUP)

    raw_loads = []
    for d in (2, 1, 3, 0):
        fi = wrap(x + d)
        copy = pltpu.make_async_copy(
            grads_m.at[:, group_cols(fi)], raw_m.at[:, group_cols(fi)], load_sem.at[d]
        )
        copy.start()
        raw_loads.append(copy)

    barrier = pltpu.get_barrier_semaphore()
    near_z = ({"z": lax.rem(z + 1, 8)}, {"z": lax.rem(z + 7, 8)})
    for peer in (
        {"x": wrap(x + 1)}, {"x": wrap(x + 3)}, {"y": wrap(y + 1)}, {"y": wrap(y + 3)}, *near_z
    ):
        pl.semaphore_signal(barrier, inc=1, device_id=peer, device_id_type=MESH_ID)

    @pl.when(c == 0)
    def _():
        pl.semaphore_signal(barrier, inc=1, device_id={"c": 1}, device_id_type=MESH_ID)

    query_loads = []
    for k in range(N):
        rows = pl.ds(pl.multiple_of(wrap(x + OFFSETS[k]) * GROUP, GROUP), GROUP)
        copy = pltpu.make_async_copy(grads_q.at[rows], raw_q.at[rows], load_sem.at[4 + k])
        copy.start()
        query_loads.append(copy)
    state_loads = []
    for i, ref in enumerate(
        (accum_q, accum_m, master_q, master_m, moment_q, moment_m, second_q, second_m)
    ):
        copy = pltpu.make_async_copy(ref, state.at[i], load_sem.at[8 + min(i, 2)])
        copy.start()
        state_loads.append(copy)

    pl.semaphore_wait(barrier, 6 + c)

    def near_signal(r):
        for peer in near_z:
            pl.semaphore_signal(hand.at[r], inc=1, device_id=peer, device_id_type=MESH_ID)

    def near_wait(r):
        pl.semaphore_wait(hand.at[r], 2)

    def partner_signal():
        pl.semaphore_signal(hand.at[3], inc=1, device_id={"c": 1 - c}, device_id_type=MESH_ID)

    def remote(src, dst, send, recv, axis, coordinate):
        return pltpu.make_async_remote_copy(
            src_ref=src,
            dst_ref=dst,
            send_sem=send,
            recv_sem=recv,
            device_id={axis: coordinate},
            device_id_type=MESH_ID,
        )

    def go(copy):
        copy.start()

    source = (raw_q, turned_m)
    low, high = pl.ds(0, HALF), pl.ds(HALF, HALF)

    def place(a, k):
        fi, si = f[a], wrap(s[a] + OFFSETS[k])
        return wrap(fi + 1), wrap(fi + 3), wrap(fi + 2), si

    def rs_copy(a, k, kind):
        plus, minus, far, si = place(a, k)

        def mine(owner, start):
            return source[a].at[shard_rows(shard_index(a, owner, si), start, HALF)]

        src, dst = {
            RELAY_A: lambda: (mine(far, 0), relay.at[a, k, 0]),
            RELAY_B: lambda: (mine(far, HALF), relay.at[a, k, 1]),
            RAW_P: lambda: (mine(plus, HALF), raw_in.at[a, k, 0]),
            RAW_M: lambda: (mine(minus, 0), raw_in.at[a, k, 1]),
            SUM_P: lambda: (sum_out.at[a, k, 0], sum_in.at[a, k, 0]),
            SUM_M: lambda: (sum_out.at[a, k, 1], sum_in.at[a, k, 1]),
        }[kind]()
        target = plus if kind in (RELAY_A, RAW_P, SUM_P) else minus
        return remote(
            src, dst, rs_send.at[a], rs_recv.at[a, k, min(kind, 2)], first_axis[a], target
        )

    def wait_bytes(ref, sem):
        pltpu.make_async_copy(ref, ref, sem).wait()

    def raw_relay(a, k):
        if a == 0:
            query_loads[k].wait()
        go(rs_copy(a, k, RELAY_A))
        go(rs_copy(a, k, RELAY_B))

    def raw_direct(a, k):
        go(rs_copy(a, k, RAW_P))
        go(rs_copy(a, k, RAW_M))

    def as_f32(value):
        return value.astype(jnp.float32)

    def pass_on(a, k):
        plus, minus, far, si = place(a, k)
        for side, kind, owner, start in ((0, SUM_P, plus, 0), (1, SUM_M, minus, HALF)):
            rs_copy(a, k, RELAY_A + side).wait_recv()
            base = shard_index(a, owner, si) * ROWS + start

            def step(i, carry):
                at = pl.ds(i * 16, 16)
                mine = source[a][pl.ds(pl.multiple_of(base + i * 16, 16), 16), :]
                value = as_f32(mine) + as_f32(relay[a, k, side, at, :])
                sum_out[a, k, side, at, :] = value.astype(jnp.bfloat16)
                return carry

            each_block(HALF // 16, step, 0)
            go(rs_copy(a, k, kind))

    def turn(fi):
        def step(i, carry):
            at = pl.ds(pl.multiple_of(fi * GROUP + i * 128, 128), 128)
            turned_m[at, :] = raw_m[:, at].T
            return carry

        lax.fori_loop(0, GROUP // 128, step, 0)

    def add_up(a, k):
        wait_bytes(source[a].at[pl.ds(0, 2 * ROWS)], rs_recv.at[a, k, 2])
        if k == 3:
            state_loads[a].wait()
        base = shard_index(a, f[a], wrap(s[a] + OFFSETS[k])) * ROWS
        for h in (0, 1):
            one = (sum_in, raw_in)[h]
            two = (raw_in, sum_in)[h]

            def step(i, carry):
                at = pl.ds(i * 16, 16)
                here = pl.ds(h * HALF + i * 16, 16)
                mine = source[a][pl.ds(pl.multiple_of(base + h * HALF + i * 16, 16), 16), :]
                value = as_f32(mine) + as_f32(one[a, k, 0, at, :]) + as_f32(two[a, k, 1, at, :])
                if k == 3:
                    partial[a, 1, here, :] = value + state[a, here, :]
                elif k == 0:
                    send_s[a, h, at, :] = value.astype(jnp.bfloat16)
                elif k == 1:
                    if h == 0:
                        partial[a, 0, here, :] = value
                    else:
                        send_s[a, 2, at, :] = value.astype(jnp.bfloat16)
                else:
                    if h == 0:
                        send_s[a, 3, at, :] = value.astype(jnp.bfloat16)
                    else:
                        partial[a, 0, here, :] = value
                return carry

            each_block(HALF // 16, step, 0)

    def second_copy(a, kind):
        plus, minus = wrap(s[a] + 1), wrap(s[a] + 3)
        dst = (t_buf, u_buf, v_buf)[kind // 2].at[a, kind % 2]
        target = (plus, minus)[kind % 2]
        return remote(
            send_s.at[a, kind], dst,
            rs_send.at[a], second_recv.at[a, min(kind, 2)], second_axis[a], target,
        )

    def merge_t(a):
        for side, kind in ((0, V_P), (1, V_M)):
            second_copy(a, T_A + side).wait_recv()

            def step(i, carry):
                at = pl.ds(i * 16, 16)
                here = pl.ds(side * HALF + i * 16, 16)
                value = partial[a, 0, here, :] + as_f32(t_buf[a, side, at, :])
                send_s[a, kind, at, :] = value.astype(jnp.bfloat16)
                return carry

            each_block(HALF // 16, step, 0)
            go(second_copy(a, kind))

    def squares(value):
        return jnp.sum((value * value).reshape(-1, 8, COLS), axis=0)

    def finish(a, acc):
        wait_bytes(source[a].at[pl.ds(0, 2 * ROWS)], second_recv.at[a, 2])
        for h, one, two in ((0, v_buf, u_buf), (1, u_buf, v_buf)):
            def step(i, acc):
                at = pl.ds(i * 16, 16)
                here = pl.ds(h * HALF + i * 16, 16)
                total = partial[a, 1, here, :] + as_f32(one[a, 0, at, :]) + as_f32(two[a, 1, at, :])
                partial[a, 1, here, :] = total
                return acc + squares(total)

            acc = each_block(HALF // 16, step, acc)
        return acc

    raw_relay(0, 0)
    raw_relay(0, 1)
    raw_direct(0, 0)
    raw_relay(0, 2)
    raw_direct(0, 1)
    raw_loads[0].wait()
    turn(wrap(x + 2))
    raw_relay(1, 0)
    raw_relay(1, 1)
    near_signal(0)
    raw_loads[1].wait()
    turn(wrap(x + 1))
    raw_loads[2].wait()
    turn(wrap(x + 3))
    raw_direct(1, 0)
    raw_relay(1, 2)
    raw_direct(1, 1)
    for a in (0, 1):
        pass_on(a, 0)
    for a in (0, 1):
        pass_on(a, 1)
        raw_direct(a, 2)
    near_wait(0)
    near_signal(1)
    raw_loads[3].wait()
    turn(x)
    for a in (0, 1):
        pass_on(a, 2)
    for a in (0, 1):
        add_up(a, 0)
        go(second_copy(a, T_A))
        go(second_copy(a, T_B))
        raw_relay(a, 3)
    for a in (0, 1):
        raw_direct(a, 3)
    near_wait(1)
    near_signal(2)
    for a in (0, 1):
        add_up(a, 1)
        go(second_copy(a, U_P))
    for a in (0, 1):
        add_up(a, 2)
        go(second_copy(a, U_M))
    for a in (0, 1):
        merge_t(a)
    near_wait(2)

    @pl.when(c == 1)
    def _():
        partner_signal()

    for a in (0, 1):
        pass_on(a, 3)

    @pl.when(c == 0)
    def _():
        pl.semaphore_wait(hand.at[3], 1)
        partner_signal()

    for a in (0, 1):
        add_up(a, 3)

    acc = jnp.zeros((8, COLS), jnp.float32)
    for a in (0, 1):
        acc = finish(a, acc)

    @pl.when(c == 1)
    def _():
        pl.semaphore_wait(hand.at[3], 1)

    def exchange(stage, row, buf, me, peers):
        row_buf[stage] = row
        buf[me] = row
        for peer in peers:
            go(
                pltpu.make_async_remote_copy(
                    src_ref=row_buf.at[stage],
                    dst_ref=buf.at[me],
                    send_sem=ar_send.at[stage],
                    recv_sem=ar_recv.at[stage],
                    device_id=peer,
                    device_id_type=MESH_ID,
                )
            )
        wait_bytes(buf.at[pl.ds(0, 15)], ar_recv.at[stage])
        return jnp.sum(buf[...], axis=0)

    row = jnp.sum(acc, axis=0, keepdims=True)
    row = row[:, :128] + row[:, 128:]
    row = exchange(0, row, plane_buf, me_plane, plane_peers)
    row = exchange(1, row, column_buf, me_column, column_peers)
    sumsq = jnp.sum(row, axis=1, keepdims=True)
    clip = jnp.minimum(1.0, lax.rsqrt(sumsq / float(ENTRIES) + 1e-06))

    gathered = (weight_q, gather_m)
    outs = ((shard_q, first_q, variance_q), (shard_m, first_m, variance_m))
    pltpu.make_async_copy(state.at[pl.ds(2, 6)], state.at[pl.ds(2, 6)], load_sem.at[10]).wait()

    def update(a):
        base = shard_index(a, f[a], s[a]) * ROWS
        shard_out, first_out, variance_out = outs[a]

        def step(i, carry):
            at = pl.ds(i * BLOCK, BLOCK)
            scaled = clip * partial[a, 1, at, :]
            master = state[2 + a, at, :]
            first = BETA_ONE * state[4 + a, at, :] + (1.0 - BETA_ONE) * scaled
            variance = BETA_TWO * state[6 + a, at, :] + (1.0 - BETA_TWO) * scaled * scaled
            corr_one = 1.0 - BETA_ONE**STEP
            corr_two = 1.0 - BETA_TWO**STEP
            change = (
                first / corr_one / (jnp.sqrt(variance / corr_two) + ADAM_EPS)
                + WEIGHT_DECAY * master
            )
            shard = master - LEARN_RATE * change
            shard_out[at, :] = shard
            first_out[at, :] = first
            variance_out[at, :] = variance
            gathered[a][pl.ds(pl.multiple_of(base + i * BLOCK, BLOCK), BLOCK), :] = shard.astype(
                jnp.bfloat16
            )
            return carry

        each_block(ROWS // BLOCK, step, 0)

    ITEMS = (0, 3, 1, 2)

    def ag_copy(a, item, kind):
        if item == 0:
            axis, here = second_axis[a], s[a]
        else:
            axis, here = first_axis[a], f[a]
        owner = {2: wrap(here + 3), 3: wrap(here + 1)}.get(kind, here)
        if item == 0:
            index = shard_index(a, f[a], owner)
        else:
            index = shard_index(a, owner, wrap(s[a] + ITEMS[item - 1]))
        if item > 0 and kind < 2:
            start, size = 0, ROWS
        else:
            start, size = (HALF if kind in (1, 3, 4) else 0), HALF
        ref = gathered[a].at[shard_rows(index, start, size)]
        target = wrap(here + 1) if kind in (0, 2, 4) else wrap(here + 3)
        if kind < 2:
            slot = 2 * item + kind
        elif kind > 3:
            slot = 12
        else:
            slot = 10 if item == 0 else 11
        return remote(ref, ref, ag_send.at[a], ag_recv.at[a, slot], axis, target)

    def ag_wait(a, item, kind):
        size = HALF if item == 0 else ROWS
        wait_bytes(gathered[a].at[pl.ds(0, size)], ag_recv.at[a, 2 * item + kind])

    def ag_wait_far(a, along_first):
        count = N * ROWS if along_first else ROWS
        wait_bytes(gathered[a].at[pl.ds(0, count)], ag_recv.at[a, 11 if along_first else 10])

    def turn_back(fi):
        def step(i, carry):
            at = pl.ds(pl.multiple_of(fi * GROUP + i * 128, 128), 128)
            weight_m[:, at] = gather_m[at, :].T
            return carry

        lax.fori_loop(0, GROUP // 128, step, 0)

    for a in (0, 1):
        update(a)
        for kind in (0, 1, 4, 5):
            go(ag_copy(a, 0, kind))
    for a in (0, 1):
        go(ag_copy(a, 1, 0))
        go(ag_copy(a, 1, 1))

    def ag_forward(a, item):
        ag_wait(a, item, 0)
        go(ag_copy(a, item, 2))
        ag_wait(a, item, 1)
        go(ag_copy(a, item, 3))

    for a in (0, 1):
        ag_forward(a, 0)
    for a in (0, 1):
        wait_bytes(gathered[a].at[pl.ds(0, ROWS)], ag_recv.at[a, 12])
        for item in (2, 3):
            go(ag_copy(a, item, 0))
            go(ag_copy(a, item, 1))
    for a in (0, 1):
        ag_wait_far(a, False)
        go(ag_copy(a, 4, 0))
        go(ag_copy(a, 4, 1))
    for a in (0, 1):
        ag_forward(a, 1)
    turn_back(x)
    for item in (2, 3, 4):
        for a in (0, 1):
            ag_forward(a, item)
    turn_back(wrap(x + 1))
    turn_back(wrap(x + 3))
    ag_wait_far(1, True)
    turn_back(wrap(x + 2))
    ag_wait_far(0, True)
    for a in (0, 1):
        wait_bytes(gathered[a].at[pl.ds(0, 15 * ROWS)], ag_send.at[a])
        wait_bytes(gathered[a].at[pl.ds(0, 15 * ROWS)], rs_send.at[a])
        wait_bytes(plane_buf.at[pl.ds(0, 15)], ar_send.at[a])


def write_out(*refs):
    sources, targets, sem = refs[:8], refs[8:16], refs[16]
    copies = [
        pltpu.make_async_copy(source, target, sem.at[i])
        for i, (source, target) in enumerate(zip(sources, targets))
    ]
    for copy in copies:
        copy.start()
    for copy in copies:
        copy.wait()


def on_device(
    query_grads, merge_grads, query_accum, merge_accum, query_master, merge_master,
    query_moment, merge_moment, query_second, merge_second,
):
    def flat(value):
        return value.reshape(ROWS, COLS)

    def turned(value):
        return jnp.swapaxes(value[0], 0, 1)

    bf16, f32 = jnp.bfloat16, jnp.float32
    hbm_spec = pl.BlockSpec(memory_space=pltpu.HBM)
    shard = pltpu.VMEM((ROWS, COLS), f32)
    operands = (
        query_grads.reshape(FULL, COLS), merge_grads.reshape(COLS, FULL),
        flat(query_accum), turned(merge_accum), flat(query_master), turned(merge_master),
        flat(query_moment), turned(merge_moment), flat(query_second), turned(merge_second),
    )
    operands = [pltpu.with_memory_space_constraint(value, pltpu.HBM) for value in operands]
    outs = pl.pallas_call(
        kernel,
        name="adamw_step",
        out_shape=[
            pltpu.VMEM((FULL, COLS), bf16),
            pltpu.VMEM((COLS, FULL), bf16),
            shard, shard, shard, shard, shard, shard,
        ],
        in_specs=[hbm_spec] * 10,
        out_specs=[pl.BlockSpec(memory_space=pltpu.VMEM)] * 8,
        scratch_shapes=[
            pltpu.VMEM((COLS, FULL), bf16),
            pltpu.VMEM((FULL, COLS), bf16),
            pltpu.VMEM((FULL, COLS), bf16),
            pltpu.VMEM((2, N, 2, HALF, COLS), bf16),
            pltpu.VMEM((2, N, 2, HALF, COLS), bf16),
            pltpu.VMEM((2, N, 2, HALF, COLS), bf16),
            pltpu.VMEM((2, N, 2, HALF, COLS), bf16),
            pltpu.VMEM((2, 2, ROWS, COLS), f32),
            pltpu.VMEM((2, 6, HALF, COLS), bf16),
            pltpu.VMEM((2, 2, HALF, COLS), bf16),
            pltpu.VMEM((2, 2, HALF, COLS), bf16),
            pltpu.VMEM((2, 2, HALF, COLS), bf16),
            pltpu.VMEM((8, ROWS, COLS), f32),
            pltpu.VMEM((FULL, COLS), bf16),
            pltpu.VMEM((16, 1, 128), f32),
            pltpu.VMEM((16, 1, 128), f32),
            pltpu.VMEM((2, 1, 128), f32),
            pltpu.SemaphoreType.DMA((11,)),
            pltpu.SemaphoreType.DMA((2,)),
            pltpu.SemaphoreType.DMA((2, N, 3)),
            pltpu.SemaphoreType.DMA((2, 3)),
            pltpu.SemaphoreType.DMA((2,)),
            pltpu.SemaphoreType.DMA((2, 13)),
            pltpu.SemaphoreType.DMA((2,)),
            pltpu.SemaphoreType.DMA((2,)),
            pltpu.SemaphoreType.REGULAR((4,)),
        ],
        compiler_params=pltpu.CompilerParams(
            collective_id=0, has_side_effects=True, vmem_limit_bytes=32 * 2**20
        ),
    )(*operands)
    outs = pl.pallas_call(
        write_out,
        name="write_out",
        out_shape=[jax.ShapeDtypeStruct(out.shape, out.dtype) for out in outs],
        in_specs=[pl.BlockSpec(memory_space=pltpu.VMEM)] * 8,
        out_specs=[hbm_spec] * 8,
        scratch_shapes=[pltpu.SemaphoreType.DMA((8,))],
        compiler_params=pltpu.CompilerParams(vmem_limit_bytes=2**20),
    )(*outs)
    weight_q, weight_m, shard_q, shard_m, first_q, first_m, variance_q, variance_m = outs

    def back(value):
        return jnp.swapaxes(value, 0, 1)[None]

    return (
        weight_q[None], weight_m[None],
        shard_q[None], back(shard_m), first_q[None], back(first_m), variance_q[None], back(variance_m),
    )


def solution(mesh):
    finer = Mesh(mesh.devices.reshape(4, 4, 8, 2), ("x", "y", "z", "c"))
    dp, mp = ("x", "y"), ("z", "c")
    query, merge = P(None, dp, mp), P(None, mp, dp)
    return jax.shard_map(
        on_device,
        mesh=finer,
        in_specs=(P(dp, None, None, mp), P(dp, None, mp, None)) + (query, merge) * 4,
        out_specs=(P(None, None, mp), P(None, mp, None)) + (query, merge) * 3,
        check_vma=False,
    )
```

```python
import jax
import jax.numpy as jnp
from jax import lax
from jax.experimental import pallas as pl
from jax.experimental.pallas import tpu as pltpu
from jax.sharding import Mesh
from jax.sharding import PartitionSpec as P

STEP = 10
ENTRIES = 29360128
BETA_ONE = 0.9
BETA_TWO = 0.95
LEARN_RATE = 0.002
WEIGHT_DECAY = 0.1
ADAM_EPS = 1e-08

N = 4
ROWS = 224
COLS = 256
HALF = ROWS // 2
GROUP = N * ROWS
FULL = N * GROUP
BLOCK = 32
MESH_ID = pl.DeviceIdType.MESH
OFFSETS = (2, 1, 3, 0)

RELAY_A, RELAY_B, RAW_P, RAW_M, SUM_P, SUM_M = range(6)
T_A, T_B, U_P, U_M, V_P, V_M = range(6)


def wrap(value):
    return lax.rem(value, N)


def each_block(count, step, carry):
    for i in range(count):
        carry = step(i, carry)
    return carry


def shard_rows(index, start=0, size=ROWS):
    return pl.ds(pl.multiple_of(index * ROWS + start, 16), size)


def kernel(
    grads_q, grads_m, accum_q, accum_m, master_q, master_m, moment_q, moment_m, second_q, second_m,
    weight_q, weight_m, shard_q, shard_m, first_q, first_m, variance_q, variance_m,
    raw_m, turned_m, raw_q, relay, raw_in, sum_in, sum_out, partial, send_s, t_buf, u_buf, v_buf, state, gather_m,
    plane_buf, column_buf, row_buf,
    load_sem, rs_send, rs_recv, second_recv, ag_send, ag_recv, ar_send, ar_recv, hand,
):
    x, y = lax.axis_index("x"), lax.axis_index("y")
    z, c = lax.axis_index("z"), lax.axis_index("c")
    first_axis, second_axis = ("y", "x"), ("x", "y")
    f, s = (y, x), (x, y)

    def shard_index(a, fi, si):
        return si * N + fi if a == 0 else fi * N + si

    barrier = pltpu.get_barrier_semaphore()
    near_z = ({"z": lax.rem(z + 1, 8)}, {"z": lax.rem(z + 7, 8)})
    for peer in (
        {"x": wrap(x + 1)}, {"x": wrap(x + 3)}, {"y": wrap(y + 1)}, {"y": wrap(y + 3)}, *near_z
    ):
        pl.semaphore_signal(barrier, inc=1, device_id=peer, device_id_type=MESH_ID)

    @pl.when(c == 0)
    def _():
        pl.semaphore_signal(barrier, inc=1, device_id={"c": 1}, device_id_type=MESH_ID)

    me_plane = x * N + y
    near_first = (0, 1, 3, 2)
    plane_peers = [
        {"x": wrap(x + dx), "y": wrap(y + dy), "c": 1}
        for dx in reversed(near_first) for dy in reversed(near_first) if dx + dy > 0
    ]
    column_peers = [
        {"z": lax.rem(z + dz, 8), "c": other}
        for dz in (4, 3, 5, 2, 6, 1, 7, 0) for other in (0, 1) if dz + 1 - other > 0
    ]

    def group_cols(fi):
        return pl.ds(pl.multiple_of(fi * GROUP, 128), GROUP)

    raw_loads = []
    for d in (2, 1, 3, 0):
        fi = wrap(x + d)
        copy = pltpu.make_async_copy(
            grads_m.at[:, group_cols(fi)], raw_m.at[:, group_cols(fi)], load_sem.at[d]
        )
        copy.start()
        raw_loads.append(copy)

    query_loads = []
    for k in range(N):
        rows = pl.ds(pl.multiple_of(wrap(x + OFFSETS[k]) * GROUP, GROUP), GROUP)
        copy = pltpu.make_async_copy(grads_q.at[rows], raw_q.at[rows], load_sem.at[4 + k])
        copy.start()
        query_loads.append(copy)
    state_loads = []
    for i, ref in enumerate(
        (accum_q, accum_m, master_q, master_m, moment_q, moment_m, second_q, second_m)
    ):
        copy = pltpu.make_async_copy(ref, state.at[i], load_sem.at[8 + min(i, 2)])
        copy.start()
        state_loads.append(copy)

    def turn(fi):
        def step(i, carry):
            at = pl.ds(pl.multiple_of(fi * GROUP + i * 128, 128), 128)
            turned_m[at, :] = raw_m[:, at].T
            return carry

        lax.fori_loop(0, GROUP // 128, step, 0)

    raw_loads[0].wait()
    turn(wrap(x + 2))
    pl.semaphore_wait(barrier, 6 + c)

    def near_signal(r):
        for peer in near_z:
            pl.semaphore_signal(hand.at[r], inc=1, device_id=peer, device_id_type=MESH_ID)

    def near_wait(r):
        pl.semaphore_wait(hand.at[r], 2)

    def partner_signal():
        pl.semaphore_signal(hand.at[3], inc=1, device_id={"c": 1 - c}, device_id_type=MESH_ID)

    def remote(src, dst, send, recv, axis, coordinate):
        return pltpu.make_async_remote_copy(
            src_ref=src,
            dst_ref=dst,
            send_sem=send,
            recv_sem=recv,
            device_id={axis: coordinate},
            device_id_type=MESH_ID,
        )

    def go(copy):
        copy.start()

    source = (raw_q, turned_m)
    low, high = pl.ds(0, HALF), pl.ds(HALF, HALF)

    def place(a, k):
        fi, si = f[a], wrap(s[a] + OFFSETS[k])
        return wrap(fi + 1), wrap(fi + 3), wrap(fi + 2), si

    def rs_copy(a, k, kind):
        plus, minus, far, si = place(a, k)

        def mine(owner, start):
            return source[a].at[shard_rows(shard_index(a, owner, si), start, HALF)]

        src, dst = {
            RELAY_A: lambda: (mine(far, 0), relay.at[a, k, 0]),
            RELAY_B: lambda: (mine(far, HALF), relay.at[a, k, 1]),
            RAW_P: lambda: (mine(plus, HALF), raw_in.at[a, k, 0]),
            RAW_M: lambda: (mine(minus, 0), raw_in.at[a, k, 1]),
            SUM_P: lambda: (sum_out.at[a, k, 0], sum_in.at[a, k, 0]),
            SUM_M: lambda: (sum_out.at[a, k, 1], sum_in.at[a, k, 1]),
        }[kind]()
        target = plus if kind in (RELAY_A, RAW_P, SUM_P) else minus
        return remote(
            src, dst, rs_send.at[a], rs_recv.at[a, k, 0 if kind < 2 else 1], first_axis[a], target
        )

    def wait_bytes(ref, sem):
        pltpu.make_async_copy(ref, ref, sem).wait()

    def raw_relay(a, k):
        if a == 0:
            query_loads[k].wait()
        go(rs_copy(a, k, RELAY_A))
        go(rs_copy(a, k, RELAY_B))

    def raw_direct(a, k):
        go(rs_copy(a, k, RAW_P))
        go(rs_copy(a, k, RAW_M))

    def as_f32(value):
        return value.astype(jnp.float32)

    def pass_on(a, k):
        plus, minus, far, si = place(a, k)
        wait_bytes(source[a].at[pl.ds(0, ROWS)], rs_recv.at[a, k, 0])
        for side, kind, owner, start in ((0, SUM_P, plus, 0), (1, SUM_M, minus, HALF)):
            base = shard_index(a, owner, si) * ROWS + start

            def step(i, carry):
                at = pl.ds(i * 16, 16)
                mine = source[a][pl.ds(pl.multiple_of(base + i * 16, 16), 16), :]
                value = as_f32(mine) + as_f32(relay[a, k, side, at, :])
                sum_out[a, k, side, at, :] = value.astype(jnp.bfloat16)
                return carry

            each_block(HALF // 16, step, 0)
            go(rs_copy(a, k, kind))

    def add_up(a, k):
        wait_bytes(source[a].at[pl.ds(0, 2 * ROWS)], rs_recv.at[a, k, 1])
        if k == 3:
            state_loads[a].wait()
        base = shard_index(a, f[a], wrap(s[a] + OFFSETS[k])) * ROWS
        for h in (0, 1):
            one = (sum_in, raw_in)[h]
            two = (raw_in, sum_in)[h]

            def step(i, carry):
                at = pl.ds(i * 16, 16)
                here = pl.ds(h * HALF + i * 16, 16)
                mine = source[a][pl.ds(pl.multiple_of(base + h * HALF + i * 16, 16), 16), :]
                value = as_f32(mine) + as_f32(one[a, k, 0, at, :]) + as_f32(two[a, k, 1, at, :])
                if k == 3:
                    partial[a, 1, here, :] = value + state[a, here, :]
                elif k == 0:
                    send_s[a, h, at, :] = value.astype(jnp.bfloat16)
                elif k == 1:
                    if h == 0:
                        partial[a, 0, here, :] = value
                    else:
                        send_s[a, 2, at, :] = value.astype(jnp.bfloat16)
                else:
                    if h == 0:
                        send_s[a, 3, at, :] = value.astype(jnp.bfloat16)
                    else:
                        partial[a, 0, here, :] = value
                return carry

            each_block(HALF // 16, step, 0)

    def second_copy(a, kind):
        plus, minus = wrap(s[a] + 1), wrap(s[a] + 3)
        dst = (t_buf, u_buf, v_buf)[kind // 2].at[a, kind % 2]
        target = (plus, minus)[kind % 2]
        return remote(
            send_s.at[a, kind], dst,
            rs_send.at[a], second_recv.at[a, 0 if kind < 2 else 1], second_axis[a], target,
        )

    def merge_t(a):
        wait_bytes(source[a].at[pl.ds(0, ROWS)], second_recv.at[a, 0])
        for side, kind in ((0, V_P), (1, V_M)):

            def step(i, carry):
                at = pl.ds(i * 16, 16)
                here = pl.ds(side * HALF + i * 16, 16)
                value = partial[a, 0, here, :] + as_f32(t_buf[a, side, at, :])
                send_s[a, kind, at, :] = value.astype(jnp.bfloat16)
                return carry

            each_block(HALF // 16, step, 0)
            go(second_copy(a, kind))

    def squares(value):
        return jnp.sum((value * value).reshape(-1, 8, COLS), axis=0)

    def finish(a, acc):
        wait_bytes(source[a].at[pl.ds(0, 2 * ROWS)], second_recv.at[a, 1])
        for h, one, two in ((0, v_buf, u_buf), (1, u_buf, v_buf)):
            def step(i, acc):
                at = pl.ds(i * 16, 16)
                here = pl.ds(h * HALF + i * 16, 16)
                total = partial[a, 1, here, :] + as_f32(one[a, 0, at, :]) + as_f32(two[a, 1, at, :])
                partial[a, 1, here, :] = total
                return acc + squares(total)

            acc = each_block(HALF // 16, step, acc)
        return acc

    raw_relay(0, 0)
    raw_relay(0, 1)
    raw_direct(0, 0)
    raw_relay(0, 2)
    raw_direct(0, 1)
    raw_relay(1, 0)
    raw_relay(1, 1)
    near_signal(0)
    raw_loads[1].wait()
    turn(wrap(x + 1))
    raw_loads[2].wait()
    turn(wrap(x + 3))
    raw_direct(1, 0)
    raw_relay(1, 2)
    raw_direct(1, 1)
    for a in (0, 1):
        pass_on(a, 0)
    for a in (0, 1):
        pass_on(a, 1)
        raw_direct(a, 2)
    near_wait(0)
    near_signal(1)
    raw_loads[3].wait()
    turn(x)
    for a in (0, 1):
        pass_on(a, 2)
    for a in (0, 1):
        add_up(a, 0)
        go(second_copy(a, T_A))
        go(second_copy(a, T_B))
        raw_relay(a, 3)
    for a in (0, 1):
        raw_direct(a, 3)
    near_wait(1)
    near_signal(2)
    for a in (0, 1):
        add_up(a, 1)
        go(second_copy(a, U_P))
    for a in (0, 1):
        add_up(a, 2)
        go(second_copy(a, U_M))
    for a in (0, 1):
        merge_t(a)
    near_wait(2)

    @pl.when(c == 1)
    def _():
        partner_signal()

    for a in (0, 1):
        pass_on(a, 3)

    @pl.when(c == 0)
    def _():
        pl.semaphore_wait(hand.at[3], 1)
        partner_signal()

    for a in (0, 1):
        add_up(a, 3)

    acc = jnp.zeros((8, COLS), jnp.float32)
    for a in (0, 1):
        acc = finish(a, acc)

    @pl.when(c == 1)
    def _():
        pl.semaphore_wait(hand.at[3], 1)

    def row_copy(stage, dst, peer):
        return pltpu.make_async_remote_copy(
            src_ref=row_buf.at[stage],
            dst_ref=dst,
            send_sem=ar_send.at[stage],
            recv_sem=ar_recv.at[stage],
            device_id=peer,
            device_id_type=MESH_ID,
        )

    row = jnp.sum(acc, axis=0, keepdims=True)
    row = row[:, :128] + row[:, 128:]
    row_buf[0] = row
    for peer in plane_peers:
        go(row_copy(0, plane_buf.at[c * 16 + me_plane], peer))

    @pl.when(c == 0)
    def _():
        go(row_copy(0, plane_buf.at[c * 16 + me_plane], {"c": 1}))
        wait_bytes(column_buf, ar_recv.at[1])

    @pl.when(c == 1)
    def _():
        plane_buf[16 + me_plane] = row
        wait_bytes(plane_buf.at[pl.ds(0, 31)], ar_recv.at[0])
        plane_row = jnp.sum(plane_buf[...], axis=0)
        row_buf[1] = plane_row
        column_buf[z] = plane_row
        for peer in column_peers:
            go(row_copy(1, column_buf.at[z], peer))
        wait_bytes(column_buf.at[pl.ds(0, 7)], ar_recv.at[1])

    row = jnp.sum(column_buf[...], axis=0)
    sumsq = jnp.sum(row, axis=1, keepdims=True)
    clip = jnp.minimum(1.0, lax.rsqrt(sumsq / float(ENTRIES) + 1e-06))

    gathered = (weight_q, gather_m)
    outs = ((shard_q, first_q, variance_q), (shard_m, first_m, variance_m))
    pltpu.make_async_copy(state.at[pl.ds(2, 6)], state.at[pl.ds(2, 6)], load_sem.at[10]).wait()

    def update(a):
        base = shard_index(a, f[a], s[a]) * ROWS
        shard_out, first_out, variance_out = outs[a]

        def step(i, carry):
            at = pl.ds(i * BLOCK, BLOCK)
            scaled = clip * partial[a, 1, at, :]
            master = state[2 + a, at, :]
            first = BETA_ONE * state[4 + a, at, :] + (1.0 - BETA_ONE) * scaled
            variance = BETA_TWO * state[6 + a, at, :] + (1.0 - BETA_TWO) * scaled * scaled
            corr_one = 1.0 - BETA_ONE**STEP
            corr_two = 1.0 - BETA_TWO**STEP
            change = (
                first / corr_one / (jnp.sqrt(variance / corr_two) + ADAM_EPS)
                + WEIGHT_DECAY * master
            )
            shard = master - LEARN_RATE * change
            shard_out[at, :] = shard
            first_out[at, :] = first
            variance_out[at, :] = variance
            gathered[a][pl.ds(pl.multiple_of(base + i * BLOCK, BLOCK), BLOCK), :] = shard.astype(
                jnp.bfloat16
            )
            return carry

        each_block(ROWS // BLOCK, step, 0)

    ITEMS = (0, 3, 1, 2)

    def ag_copy(a, item, kind):
        if item == 0:
            axis, here = second_axis[a], s[a]
        else:
            axis, here = first_axis[a], f[a]
        owner = {2: wrap(here + 3), 3: wrap(here + 1)}.get(kind, here)
        if item == 0:
            index = shard_index(a, f[a], owner)
        else:
            index = shard_index(a, owner, wrap(s[a] + ITEMS[item - 1]))
        if item > 0 and kind < 2:
            start, size = 0, ROWS
        else:
            start, size = (HALF if kind in (1, 3, 4) else 0), HALF
        ref = gathered[a].at[shard_rows(index, start, size)]
        target = wrap(here + 1) if kind in (0, 2, 4) else wrap(here + 3)
        if kind < 2:
            slot = item
        elif kind > 3:
            slot = 5
        elif item == 0:
            slot = 6
        else:
            slot = 8 if item == 4 else 7
        return remote(ref, ref, ag_send.at[a], ag_recv.at[a, slot], axis, target)

    def ag_wait(a, slot, shards):
        wait_bytes(gathered[a].at[pl.ds(0, shards * ROWS)], ag_recv.at[a, slot])

    def turn_back(fi, count=GROUP // 128, tile=0):
        def step(i, carry):
            at = pl.ds(pl.multiple_of(fi * GROUP + lax.rem(tile + i, 7) * 128, 128), 128)
            weight_m[:, at] = gather_m[at, :].T
            return carry

        lax.fori_loop(0, count, step, 0)

    for a in (0, 1):
        update(a)
        for kind in (0, 1, 4, 5):
            go(ag_copy(a, 0, kind))
    for a in (0, 1):
        go(ag_copy(a, 1, 0))
        go(ag_copy(a, 1, 1))

    def ag_forward(a, item):
        ag_wait(a, item, 1 if item == 0 else 2)
        go(ag_copy(a, item, 2))
        go(ag_copy(a, item, 3))

    for a in (0, 1):
        ag_forward(a, 0)
    for a in (0, 1):
        ag_wait(a, 5, 1)
        for item in (2, 3):
            go(ag_copy(a, item, 0))
            go(ag_copy(a, item, 1))
    for a in (0, 1):
        ag_wait(a, 6, 1)
        go(ag_copy(a, 4, 0))
        go(ag_copy(a, 4, 1))
    for a in (0, 1):
        ag_forward(a, 1)
    turn_back(x)
    for item in (2, 3, 4):
        for a in (0, 1):
            ag_forward(a, item)
    turn_back(wrap(x + 1))
    turn_back(wrap(x + 3))
    ag_wait(1, 7, 3)
    across = wrap(y + 2)
    window = across * 7 // 4 - across // 3
    turn_back(wrap(x + 2), 4, window + 3)
    ag_wait(1, 8, 1)
    turn_back(wrap(x + 2), 3, window)
    ag_wait(0, 7, 3)
    ag_wait(0, 8, 1)
    for a in (0, 1):
        wait_bytes(gathered[a].at[pl.ds(0, 15 * ROWS)], ag_send.at[a])
        wait_bytes(gathered[a].at[pl.ds(0, 15 * ROWS)], rs_send.at[a])

    @pl.when(c == 0)
    def _():
        wait_bytes(plane_buf.at[pl.ds(0, 16)], ar_send.at[0])

    @pl.when(c == 1)
    def _():
        wait_bytes(plane_buf.at[pl.ds(0, 15)], ar_send.at[0])
        wait_bytes(plane_buf.at[pl.ds(0, 15)], ar_send.at[1])


def write_out(*refs):
    sources, targets, sem = refs[:8], refs[8:16], refs[16]
    copies = [
        pltpu.make_async_copy(source, target, sem.at[i])
        for i, (source, target) in enumerate(zip(sources, targets))
    ]
    for copy in copies:
        copy.start()
    for copy in copies:
        copy.wait()


def on_device(
    query_grads, merge_grads, query_accum, merge_accum, query_master, merge_master,
    query_moment, merge_moment, query_second, merge_second,
):
    def flat(value):
        return value.reshape(ROWS, COLS)

    def turned(value):
        return jnp.swapaxes(value[0], 0, 1)

    bf16, f32 = jnp.bfloat16, jnp.float32
    hbm_spec = pl.BlockSpec(memory_space=pltpu.HBM)
    shard = pltpu.VMEM((ROWS, COLS), f32)
    operands = (
        query_grads.reshape(FULL, COLS), merge_grads.reshape(COLS, FULL),
        flat(query_accum), turned(merge_accum), flat(query_master), turned(merge_master),
        flat(query_moment), turned(merge_moment), flat(query_second), turned(merge_second),
    )
    operands = [pltpu.with_memory_space_constraint(value, pltpu.HBM) for value in operands]
    outs = pl.pallas_call(
        kernel,
        name="adamw_step",
        out_shape=[
            pltpu.VMEM((FULL, COLS), bf16),
            pltpu.VMEM((COLS, FULL), bf16),
            shard, shard, shard, shard, shard, shard,
        ],
        in_specs=[hbm_spec] * 10,
        out_specs=[pl.BlockSpec(memory_space=pltpu.VMEM)] * 8,
        scratch_shapes=[
            pltpu.VMEM((COLS, FULL), bf16),
            pltpu.VMEM((FULL, COLS), bf16),
            pltpu.VMEM((FULL, COLS), bf16),
            pltpu.VMEM((2, N, 2, HALF, COLS), bf16),
            pltpu.VMEM((2, N, 2, HALF, COLS), bf16),
            pltpu.VMEM((2, N, 2, HALF, COLS), bf16),
            pltpu.VMEM((2, N, 2, HALF, COLS), bf16),
            pltpu.VMEM((2, 2, ROWS, COLS), f32),
            pltpu.VMEM((2, 6, HALF, COLS), bf16),
            pltpu.VMEM((2, 2, HALF, COLS), bf16),
            pltpu.VMEM((2, 2, HALF, COLS), bf16),
            pltpu.VMEM((2, 2, HALF, COLS), bf16),
            pltpu.VMEM((8, ROWS, COLS), f32),
            pltpu.VMEM((FULL, COLS), bf16),
            pltpu.VMEM((32, 1, 128), f32),
            pltpu.VMEM((8, 1, 128), f32),
            pltpu.VMEM((2, 1, 128), f32),
            pltpu.SemaphoreType.DMA((11,)),
            pltpu.SemaphoreType.DMA((2,)),
            pltpu.SemaphoreType.DMA((2, N, 2)),
            pltpu.SemaphoreType.DMA((2, 2)),
            pltpu.SemaphoreType.DMA((2,)),
            pltpu.SemaphoreType.DMA((2, 9)),
            pltpu.SemaphoreType.DMA((2,)),
            pltpu.SemaphoreType.DMA((2,)),
            pltpu.SemaphoreType.REGULAR((4,)),
        ],
        compiler_params=pltpu.CompilerParams(
            collective_id=0, has_side_effects=True, vmem_limit_bytes=32 * 2**20
        ),
    )(*operands)
    outs = pl.pallas_call(
        write_out,
        name="write_out",
        out_shape=[jax.ShapeDtypeStruct(out.shape, out.dtype) for out in outs],
        in_specs=[pl.BlockSpec(memory_space=pltpu.VMEM)] * 8,
        out_specs=[hbm_spec] * 8,
        scratch_shapes=[pltpu.SemaphoreType.DMA((8,))],
        compiler_params=pltpu.CompilerParams(vmem_limit_bytes=2**20),
    )(*outs)
    weight_q, weight_m, shard_q, shard_m, first_q, first_m, variance_q, variance_m = outs

    def back(value):
        return jnp.swapaxes(value, 0, 1)[None]

    return (
        weight_q[None], weight_m[None],
        shard_q[None], back(shard_m), first_q[None], back(first_m), variance_q[None], back(variance_m),
    )


def solution(mesh):
    finer = Mesh(mesh.devices.reshape(4, 4, 8, 2), ("x", "y", "z", "c"))
    dp, mp = ("x", "y"), ("z", "c")
    query, merge = P(None, dp, mp), P(None, mp, dp)
    return jax.shard_map(
        on_device,
        mesh=finer,
        in_specs=(P(dp, None, None, mp), P(dp, None, mp, None)) + (query, merge) * 4,
        out_specs=(P(None, None, mp), P(None, mp, None)) + (query, merge) * 3,
        check_vma=False,
    )
```

```python
import jax
import jax.numpy as jnp
from jax import lax
from jax.experimental import pallas as pl
from jax.experimental.pallas import tpu as pltpu
from jax.sharding import Mesh
from jax.sharding import PartitionSpec as P

STEP = 10
ENTRIES = 29360128
BETA_ONE = 0.9
BETA_TWO = 0.95
LEARN_RATE = 0.002
WEIGHT_DECAY = 0.1
ADAM_EPS = 1e-08

N = 4
ROWS = 224
COLS = 256
HALF = ROWS // 2
GROUP = N * ROWS
FULL = N * GROUP
BLOCK = 32
MESH_ID = pl.DeviceIdType.MESH
OFFSETS = (2, 1, 3, 0)

RELAY_A, RELAY_B, RAW_P, RAW_M, SUM_P, SUM_M = range(6)
T_A, T_B, U_P, U_M, V_P, V_M = range(6)


def wrap(value):
    return lax.rem(value, N)


def each_block(count, step, carry):
    for i in range(count):
        carry = step(i, carry)
    return carry


def shard_rows(index, start=0, size=ROWS):
    return pl.ds(pl.multiple_of(index * ROWS + start, 16), size)


def kernel(
    grads_q, grads_m, accum_q, accum_m, master_q, master_m, moment_q, moment_m, second_q, second_m,
    weight_q, weight_m, shard_q, shard_m, first_q, first_m, variance_q, variance_m,
    raw_m, turned_m, raw_q, relay, raw_in, sum_in, sum_out, partial, send_s, t_buf, u_buf, v_buf, state, gather_m,
    plane_buf, column_buf, row_buf,
    load_sem, rs_send, rs_recv, second_recv, ag_send, ag_recv, ar_send, ar_recv, hand,
):
    x, y = lax.axis_index("x"), lax.axis_index("y")
    z, c = lax.axis_index("z"), lax.axis_index("c")
    first_axis, second_axis = ("y", "x"), ("x", "y")
    f, s = (y, x), (x, y)

    def shard_index(a, fi, si):
        return si * N + fi if a == 0 else fi * N + si

    barrier = pltpu.get_barrier_semaphore()
    near_z = ({"z": lax.rem(z + 1, 8)}, {"z": lax.rem(z + 7, 8)})
    for peer in (
        {"x": wrap(x + 1)}, {"x": wrap(x + 3)}, {"y": wrap(y + 1)}, {"y": wrap(y + 3)}, *near_z
    ):
        pl.semaphore_signal(barrier, inc=1, device_id=peer, device_id_type=MESH_ID)

    @pl.when(c == 0)
    def _():
        pl.semaphore_signal(barrier, inc=1, device_id={"c": 1}, device_id_type=MESH_ID)

    me_plane = x * N + y
    near_first = (0, 1, 3, 2)
    plane_peers = [
        {"x": wrap(x + dx), "y": wrap(y + dy), "c": 1}
        for dx in reversed(near_first) for dy in reversed(near_first) if dx + dy > 0
    ]
    column_peers = [
        {"z": lax.rem(z + dz, 8), "c": other}
        for dz in (4, 3, 5, 2, 6, 1, 7, 0) for other in (0, 1) if dz + 1 - other > 0
    ]

    def group_cols(fi):
        return pl.ds(pl.multiple_of(fi * GROUP, 128), GROUP)

    raw_loads, query_loads = [], []
    for k, d in enumerate((2, 1, 3, 0)):
        rows = pl.ds(pl.multiple_of(wrap(x + OFFSETS[k]) * GROUP, GROUP), GROUP)
        copy = pltpu.make_async_copy(grads_q.at[rows], raw_q.at[rows], load_sem.at[4 + k])
        copy.start()
        query_loads.append(copy)
        cols = group_cols(wrap(x + d))
        copy = pltpu.make_async_copy(grads_m.at[:, cols], raw_m.at[:, cols], load_sem.at[d])
        copy.start()
        raw_loads.append(copy)
    state_loads = []
    for i, ref in enumerate(
        (accum_q, accum_m, master_q, master_m, moment_q, moment_m, second_q, second_m)
    ):
        copy = pltpu.make_async_copy(ref, state.at[i], load_sem.at[8 + min(i, 2)])
        copy.start()
        state_loads.append(copy)

    def turn(fi):
        def step(i, carry):
            at = pl.ds(pl.multiple_of(fi * GROUP + i * 128, 128), 128)
            turned_m[at, :] = raw_m[:, at].T
            return carry

        lax.fori_loop(0, GROUP // 128, step, 0)

    raw_loads[0].wait()
    turn(wrap(x + 2))
    pl.semaphore_wait(barrier, 6 + c)

    def near_signal(r):
        for peer in near_z:
            pl.semaphore_signal(hand.at[r], inc=1, device_id=peer, device_id_type=MESH_ID)

    def near_wait(r):
        pl.semaphore_wait(hand.at[r], 2)

    def partner_signal():
        pl.semaphore_signal(hand.at[3], inc=1, device_id={"c": 1 - c}, device_id_type=MESH_ID)

    def remote(src, dst, send, recv, axis, coordinate):
        return pltpu.make_async_remote_copy(
            src_ref=src,
            dst_ref=dst,
            send_sem=send,
            recv_sem=recv,
            device_id={axis: coordinate},
            device_id_type=MESH_ID,
        )

    def go(copy):
        copy.start()

    source = (raw_q, turned_m)
    low, high = pl.ds(0, HALF), pl.ds(HALF, HALF)

    def place(a, k):
        fi, si = f[a], wrap(s[a] + OFFSETS[k])
        return wrap(fi + 1), wrap(fi + 3), wrap(fi + 2), si

    def rs_copy(a, k, kind):
        plus, minus, far, si = place(a, k)

        def mine(owner, start):
            return source[a].at[shard_rows(shard_index(a, owner, si), start, HALF)]

        src, dst = {
            RELAY_A: lambda: (mine(far, 0), relay.at[a, k, 0]),
            RELAY_B: lambda: (mine(far, HALF), relay.at[a, k, 1]),
            RAW_P: lambda: (mine(plus, HALF), raw_in.at[a, k, 0]),
            RAW_M: lambda: (mine(minus, 0), raw_in.at[a, k, 1]),
            SUM_P: lambda: (sum_out.at[a, k, 0], sum_in.at[a, k, 0]),
            SUM_M: lambda: (sum_out.at[a, k, 1], sum_in.at[a, k, 1]),
        }[kind]()
        target = plus if kind in (RELAY_A, RAW_P, SUM_P) else minus
        return remote(
            src, dst, rs_send.at[a], rs_recv.at[a, k, 0 if kind < 2 else 1], first_axis[a], target
        )

    def wait_bytes(ref, sem):
        pltpu.make_async_copy(ref, ref, sem).wait()

    def raw_relay(a, k):
        if a == 0:
            query_loads[k].wait()
        go(rs_copy(a, k, RELAY_A))
        go(rs_copy(a, k, RELAY_B))

    def raw_direct(a, k):
        go(rs_copy(a, k, RAW_P))
        go(rs_copy(a, k, RAW_M))

    def as_f32(value):
        return value.astype(jnp.float32)

    def pass_on(a, k):
        plus, minus, far, si = place(a, k)
        wait_bytes(source[a].at[pl.ds(0, ROWS)], rs_recv.at[a, k, 0])
        for side, kind, owner, start in ((0, SUM_P, plus, 0), (1, SUM_M, minus, HALF)):
            base = shard_index(a, owner, si) * ROWS + start

            def step(i, carry):
                at = pl.ds(i * 16, 16)
                mine = source[a][pl.ds(pl.multiple_of(base + i * 16, 16), 16), :]
                value = as_f32(mine) + as_f32(relay[a, k, side, at, :])
                sum_out[a, k, side, at, :] = value.astype(jnp.bfloat16)
                return carry

            each_block(HALF // 16, step, 0)
            go(rs_copy(a, k, kind))

    def add_up(a, k):
        wait_bytes(source[a].at[pl.ds(0, 2 * ROWS)], rs_recv.at[a, k, 1])
        if k == 3:
            state_loads[a].wait()
        base = shard_index(a, f[a], wrap(s[a] + OFFSETS[k])) * ROWS
        for h in (0, 1):
            one = (sum_in, raw_in)[h]
            two = (raw_in, sum_in)[h]

            def step(i, carry):
                at = pl.ds(i * 16, 16)
                here = pl.ds(h * HALF + i * 16, 16)
                mine = source[a][pl.ds(pl.multiple_of(base + h * HALF + i * 16, 16), 16), :]
                value = as_f32(mine) + as_f32(one[a, k, 0, at, :]) + as_f32(two[a, k, 1, at, :])
                if k == 3:
                    partial[a, 1, here, :] = value + state[a, here, :]
                elif k == 0:
                    send_s[a, h, at, :] = value.astype(jnp.bfloat16)
                elif k == 1:
                    if h == 0:
                        partial[a, 0, here, :] = value
                    else:
                        send_s[a, 2, at, :] = value.astype(jnp.bfloat16)
                else:
                    if h == 0:
                        send_s[a, 3, at, :] = value.astype(jnp.bfloat16)
                    else:
                        partial[a, 0, here, :] = value
                return carry

            each_block(HALF // 16, step, 0)

    def second_copy(a, kind):
        plus, minus = wrap(s[a] + 1), wrap(s[a] + 3)
        dst = (t_buf, u_buf, v_buf)[kind // 2].at[a, kind % 2]
        target = (plus, minus)[kind % 2]
        return remote(
            send_s.at[a, kind], dst,
            rs_send.at[a], second_recv.at[a, 0 if kind < 2 else 1], second_axis[a], target,
        )

    def merge_t(a):
        wait_bytes(source[a].at[pl.ds(0, ROWS)], second_recv.at[a, 0])
        for side, kind in ((0, V_P), (1, V_M)):

            def step(i, carry):
                at = pl.ds(i * 16, 16)
                here = pl.ds(side * HALF + i * 16, 16)
                value = partial[a, 0, here, :] + as_f32(t_buf[a, side, at, :])
                send_s[a, kind, at, :] = value.astype(jnp.bfloat16)
                return carry

            each_block(HALF // 16, step, 0)
            go(second_copy(a, kind))

    def squares(value):
        return jnp.sum((value * value).reshape(-1, 8, COLS), axis=0)

    def finish(a, acc):
        wait_bytes(source[a].at[pl.ds(0, 2 * ROWS)], second_recv.at[a, 1])
        for h, one, two in ((0, v_buf, u_buf), (1, u_buf, v_buf)):
            def step(i, acc):
                at = pl.ds(i * 16, 16)
                here = pl.ds(h * HALF + i * 16, 16)
                total = partial[a, 1, here, :] + as_f32(one[a, 0, at, :]) + as_f32(two[a, 1, at, :])
                partial[a, 1, here, :] = total
                return acc + squares(total)

            acc = each_block(HALF // 16, step, acc)
        return acc

    raw_relay(0, 0)
    raw_relay(0, 1)
    raw_direct(0, 0)
    raw_relay(0, 2)
    raw_direct(0, 1)
    raw_relay(1, 0)
    raw_relay(1, 1)
    near_signal(0)
    raw_loads[1].wait()
    turn(wrap(x + 1))
    raw_loads[2].wait()
    turn(wrap(x + 3))
    raw_direct(1, 0)
    raw_relay(1, 2)
    raw_direct(1, 1)
    for a in (0, 1):
        pass_on(a, 0)
    for a in (0, 1):
        pass_on(a, 1)
        raw_direct(a, 2)
    near_wait(0)
    near_signal(1)
    raw_loads[3].wait()
    turn(x)
    for a in (0, 1):
        pass_on(a, 2)
        raw_relay(a, 3)
    for a in (0, 1):
        add_up(a, 0)
        go(second_copy(a, T_A))
        go(second_copy(a, T_B))
    for a in (0, 1):
        raw_direct(a, 3)
    near_wait(1)
    near_signal(2)
    for a in (0, 1):
        add_up(a, 1)
        go(second_copy(a, U_P))
    for a in (0, 1):
        add_up(a, 2)
        go(second_copy(a, U_M))
    for a in (0, 1):
        pass_on(a, 3)
    for a in (0, 1):
        merge_t(a)
    near_wait(2)

    @pl.when(c == 1)
    def _():
        partner_signal()

    @pl.when(c == 0)
    def _():
        pl.semaphore_wait(hand.at[3], 1)
        partner_signal()

    for a in (0, 1):
        add_up(a, 3)

    acc = jnp.zeros((8, COLS), jnp.float32)
    for a in (0, 1):
        acc = finish(a, acc)

    @pl.when(c == 1)
    def _():
        pl.semaphore_wait(hand.at[3], 1)

    def row_copy(stage, dst, peer):
        return pltpu.make_async_remote_copy(
            src_ref=row_buf.at[stage],
            dst_ref=dst,
            send_sem=ar_send.at[stage],
            recv_sem=ar_recv.at[stage],
            device_id=peer,
            device_id_type=MESH_ID,
        )

    row = jnp.sum(acc, axis=0, keepdims=True)
    row = row[:, :128] + row[:, 128:]
    row_buf[0] = row
    for peer in plane_peers:
        go(row_copy(0, plane_buf.at[c * 16 + me_plane], peer))

    @pl.when(c == 0)
    def _():
        go(row_copy(0, plane_buf.at[c * 16 + me_plane], {"c": 1}))
        wait_bytes(column_buf, ar_recv.at[1])

    @pl.when(c == 1)
    def _():
        plane_buf[16 + me_plane] = row
        wait_bytes(plane_buf.at[pl.ds(0, 31)], ar_recv.at[0])
        plane_row = jnp.sum(plane_buf[...], axis=0)
        row_buf[1] = plane_row
        column_buf[z] = plane_row
        for peer in column_peers:
            go(row_copy(1, column_buf.at[z], peer))
        wait_bytes(column_buf.at[pl.ds(0, 7)], ar_recv.at[1])

    row = jnp.sum(column_buf[...], axis=0)
    sumsq = jnp.sum(row, axis=1, keepdims=True)
    clip = jnp.minimum(1.0, lax.rsqrt(sumsq / float(ENTRIES) + 1e-06))

    gathered = (weight_q, gather_m)
    outs = ((shard_q, first_q, variance_q), (shard_m, first_m, variance_m))
    pltpu.make_async_copy(state.at[pl.ds(2, 6)], state.at[pl.ds(2, 6)], load_sem.at[10]).wait()

    def update(a):
        base = shard_index(a, f[a], s[a]) * ROWS
        shard_out, first_out, variance_out = outs[a]

        def step(i, carry):
            at = pl.ds(i * BLOCK, BLOCK)
            scaled = clip * partial[a, 1, at, :]
            master = state[2 + a, at, :]
            first = BETA_ONE * state[4 + a, at, :] + (1.0 - BETA_ONE) * scaled
            variance = BETA_TWO * state[6 + a, at, :] + (1.0 - BETA_TWO) * scaled * scaled
            corr_one = 1.0 - BETA_ONE**STEP
            corr_two = 1.0 - BETA_TWO**STEP
            change = (
                first / corr_one / (jnp.sqrt(variance / corr_two) + ADAM_EPS)
                + WEIGHT_DECAY * master
            )
            shard = master - LEARN_RATE * change
            shard_out[at, :] = shard
            first_out[at, :] = first
            variance_out[at, :] = variance
            gathered[a][pl.ds(pl.multiple_of(base + i * BLOCK, BLOCK), BLOCK), :] = shard.astype(
                jnp.bfloat16
            )
            return carry

        each_block(ROWS // BLOCK, step, 0)

    ITEMS = (0, 3, 1, 2)

    def ag_copy(a, item, kind):
        if item == 0:
            axis, here = second_axis[a], s[a]
        else:
            axis, here = first_axis[a], f[a]
        owner = {2: wrap(here + 3), 3: wrap(here + 1)}.get(kind, here)
        if item == 0:
            index = shard_index(a, f[a], owner)
        else:
            index = shard_index(a, owner, wrap(s[a] + ITEMS[item - 1]))
        if item > 0 and kind < 2:
            start, size = 0, ROWS
        else:
            start, size = (HALF if kind in (1, 3, 4) else 0), HALF
        ref = gathered[a].at[shard_rows(index, start, size)]
        target = wrap(here + 1) if kind in (0, 2, 4) else wrap(here + 3)
        if kind < 2:
            slot = item
        elif kind > 3:
            slot = 5
        elif item == 0:
            slot = 6
        else:
            slot = 8 if item == 4 else 7
        return remote(ref, ref, ag_send.at[a], ag_recv.at[a, slot], axis, target)

    def ag_wait(a, slot, shards):
        wait_bytes(gathered[a].at[pl.ds(0, shards * ROWS)], ag_recv.at[a, slot])

    def turn_back(fi, count=GROUP // 128, tile=0):
        def step(i, carry):
            at = pl.ds(pl.multiple_of(fi * GROUP + lax.rem(tile + i, 7) * 128, 128), 128)
            weight_m[:, at] = gather_m[at, :].T
            return carry

        lax.fori_loop(0, count, step, 0)

    for a in (0, 1):
        update(a)
        for kind in (0, 1, 4, 5):
            go(ag_copy(a, 0, kind))
    for a in (0, 1):
        go(ag_copy(a, 1, 0))
        go(ag_copy(a, 1, 1))

    def ag_forward(a, item):
        ag_wait(a, item, 1 if item == 0 else 2)
        go(ag_copy(a, item, 2))
        go(ag_copy(a, item, 3))

    for a in (0, 1):
        ag_forward(a, 0)
    for a in (0, 1):
        ag_wait(a, 5, 1)
        for item in (2, 3):
            go(ag_copy(a, item, 0))
            go(ag_copy(a, item, 1))
    for a in (0, 1):
        ag_wait(a, 6, 1)
        go(ag_copy(a, 4, 0))
        go(ag_copy(a, 4, 1))
    for a in (0, 1):
        ag_forward(a, 1)
    turn_back(x)
    for item in (2, 3, 4):
        for a in (0, 1):
            ag_forward(a, item)
    turn_back(wrap(x + 1))
    turn_back(wrap(x + 3))
    ag_wait(1, 7, 3)
    across = wrap(y + 2)
    window = across * 7 // 4 - across // 3
    turn_back(wrap(x + 2), 4, window + 3)
    ag_wait(1, 8, 1)
    turn_back(wrap(x + 2), 3, window)
    ag_wait(0, 7, 3)
    ag_wait(0, 8, 1)
    for a in (0, 1):
        wait_bytes(gathered[a].at[pl.ds(0, 15 * ROWS)], ag_send.at[a])
        wait_bytes(gathered[a].at[pl.ds(0, 15 * ROWS)], rs_send.at[a])

    @pl.when(c == 0)
    def _():
        wait_bytes(plane_buf.at[pl.ds(0, 16)], ar_send.at[0])

    @pl.when(c == 1)
    def _():
        wait_bytes(plane_buf.at[pl.ds(0, 15)], ar_send.at[0])
        wait_bytes(plane_buf.at[pl.ds(0, 15)], ar_send.at[1])


def write_out(*refs):
    sources, targets, sem = refs[:8], refs[8:16], refs[16]
    copies = [
        pltpu.make_async_copy(source, target, sem.at[min(i, 2)])
        for i, (source, target) in enumerate(zip(sources, targets))
    ]
    for copy in copies:
        copy.start()
    for copy in copies[:2]:
        copy.wait()
    whole = sources[0].at[pl.ds(0, 12 * ROWS)]
    pltpu.make_async_copy(whole, whole, sem.at[2]).wait()


def on_device(
    query_grads, merge_grads, query_accum, merge_accum, query_master, merge_master,
    query_moment, merge_moment, query_second, merge_second,
):
    def flat(value):
        return value.reshape(ROWS, COLS)

    def turned(value):
        return jnp.swapaxes(value[0], 0, 1)

    bf16, f32 = jnp.bfloat16, jnp.float32
    hbm_spec = pl.BlockSpec(memory_space=pltpu.HBM)
    shard = pltpu.VMEM((ROWS, COLS), f32)
    operands = (
        query_grads.reshape(FULL, COLS), merge_grads.reshape(COLS, FULL),
        flat(query_accum), turned(merge_accum), flat(query_master), turned(merge_master),
        flat(query_moment), turned(merge_moment), flat(query_second), turned(merge_second),
    )
    operands = [pltpu.with_memory_space_constraint(value, pltpu.HBM) for value in operands]
    outs = pl.pallas_call(
        kernel,
        name="adamw_step",
        out_shape=[
            pltpu.VMEM((FULL, COLS), bf16),
            pltpu.VMEM((COLS, FULL), bf16),
            shard, shard, shard, shard, shard, shard,
        ],
        in_specs=[hbm_spec] * 10,
        out_specs=[pl.BlockSpec(memory_space=pltpu.VMEM)] * 8,
        scratch_shapes=[
            pltpu.VMEM((COLS, FULL), bf16),
            pltpu.VMEM((FULL, COLS), bf16),
            pltpu.VMEM((FULL, COLS), bf16),
            pltpu.VMEM((2, N, 2, HALF, COLS), bf16),
            pltpu.VMEM((2, N, 2, HALF, COLS), bf16),
            pltpu.VMEM((2, N, 2, HALF, COLS), bf16),
            pltpu.VMEM((2, N, 2, HALF, COLS), bf16),
            pltpu.VMEM((2, 2, ROWS, COLS), f32),
            pltpu.VMEM((2, 6, HALF, COLS), bf16),
            pltpu.VMEM((2, 2, HALF, COLS), bf16),
            pltpu.VMEM((2, 2, HALF, COLS), bf16),
            pltpu.VMEM((2, 2, HALF, COLS), bf16),
            pltpu.VMEM((8, ROWS, COLS), f32),
            pltpu.VMEM((FULL, COLS), bf16),
            pltpu.VMEM((32, 1, 128), f32),
            pltpu.VMEM((8, 1, 128), f32),
            pltpu.VMEM((2, 1, 128), f32),
            pltpu.SemaphoreType.DMA((11,)),
            pltpu.SemaphoreType.DMA((2,)),
            pltpu.SemaphoreType.DMA((2, N, 2)),
            pltpu.SemaphoreType.DMA((2, 2)),
            pltpu.SemaphoreType.DMA((2,)),
            pltpu.SemaphoreType.DMA((2, 9)),
            pltpu.SemaphoreType.DMA((2,)),
            pltpu.SemaphoreType.DMA((2,)),
            pltpu.SemaphoreType.REGULAR((4,)),
        ],
        compiler_params=pltpu.CompilerParams(
            collective_id=0, has_side_effects=True, vmem_limit_bytes=32 * 2**20
        ),
    )(*operands)
    outs = pl.pallas_call(
        write_out,
        name="write_out",
        out_shape=[jax.ShapeDtypeStruct(out.shape, out.dtype) for out in outs],
        in_specs=[pl.BlockSpec(memory_space=pltpu.VMEM)] * 8,
        out_specs=[hbm_spec] * 8,
        scratch_shapes=[pltpu.SemaphoreType.DMA((3,))],
        compiler_params=pltpu.CompilerParams(vmem_limit_bytes=2**20),
    )(*outs)
    weight_q, weight_m, shard_q, shard_m, first_q, first_m, variance_q, variance_m = outs

    def back(value):
        return jnp.swapaxes(value, 0, 1)[None]

    return (
        weight_q[None], weight_m[None],
        shard_q[None], back(shard_m), first_q[None], back(first_m), variance_q[None], back(variance_m),
    )


def solution(mesh):
    finer = Mesh(mesh.devices.reshape(4, 4, 8, 2), ("x", "y", "z", "c"))
    dp, mp = ("x", "y"), ("z", "c")
    query, merge = P(None, dp, mp), P(None, mp, dp)
    return jax.shard_map(
        on_device,
        mesh=finer,
        in_specs=(P(dp, None, None, mp), P(dp, None, mp, None)) + (query, merge) * 4,
        out_specs=(P(None, None, mp), P(None, mp, None)) + (query, merge) * 3,
        check_vma=False,
    )
```
